256 devices in a mesh: grp: 16 (over y_hi, x, core), sub: 16 (over y_lo, z).
Axes of the slice: x: 4, y: 4 (y_hi: 2, y_lo: 2; y = y_hi * 2 + y_lo), z: 8, core: 2. Of those that a mesh axis runs over, the one named last changes fastest.
Arguments:
- arrivals: float32 [128, 262144], P('sub', 'grp'), may hold values from -64 to 64
- sketch: float32 [256, 262144], P(None, ('grp', 'sub')), may hold values from -96 to 96
- owner: int32 [8192], P('grp'), may hold values from 0 to 511, as said below
- slot: int32 [128], replicated, may hold values from 0 to 127, each once
Outputs:
- final_sketch: float32 [256, 262144], P(None, ('grp', 'sub'))
- residual: float32 [128, 262144], P(None, ('grp', 'sub'))
The draws below stay inside these ranges and needn't reach their ends.
Inputs may be any that keep to these rules, and one draw needn't show every extreme that they name: `owner`: each aligned block of 512 entries names each host of its group once. `slot`: each time step has its own arrival row.
All inputs are finite; a program needn't handle non-finite values.
Results may differ from the reference program's by a relative error of at most 0.00016.
Values sent between devices are 32-bit elements; how exact they have to be, the bound alone decides.
A program may use at most 64 MiB of HBM per device.

```python
import math
import jax
import jax.numpy as jnp
from jax import lax

HOSTS = 8192
CNT = 32
ELL = 256
NEW = 64
TOP = 32
COUNTERS = 262144
HOSTS_GRP = 512
SAMPLES = 128
N_GRP = 16


def hosts_table(key):
    anchor = jax.random.fold_in(key, 7)

    def single(index):
        return jax.random.permutation(jax.random.fold_in(anchor, index), HOSTS_GRP)
    return jax.vmap(single)(jnp.arange(HOSTS // HOSTS_GRP)).astype(jnp.int32)


def sketch_values(key):
    anchor = jax.random.fold_in(key, 11)
    coupling = jnp.clip(jax.random.normal(jax.random.fold_in(anchor, 3), (ELL, ELL)), -4.0, 4.0) / math.sqrt(ELL)
    scales = jnp.exp(jax.random.uniform(jax.random.fold_in(anchor, 1), (ELL, 1), minval=0.0, maxval=math.log(4.0)))
    values = jnp.clip(jax.random.normal(jax.random.fold_in(anchor, 2), (ELL, COUNTERS)), -6.0, 6.0)
    mixed = values + 0.25 * jnp.dot(coupling, values)
    return jnp.clip(scales * mixed, -96.0, 96.0).astype(jnp.float32)


def draw_sketch(key, part):
    return sketch_values(key)


def draw_owner(key, part):
    return hosts_table(key).reshape(HOSTS)


def draw_arrivals(key, part):
    sketch_rows = sketch_values(key)
    anchor = jax.random.fold_in(key, 13)
    mixing = jnp.clip(jax.random.normal(jax.random.fold_in(anchor, 1), (SAMPLES, ELL)), -4.0, 4.0) / math.sqrt(ELL)
    jitter = jnp.clip(jax.random.normal(jax.random.fold_in(anchor, 2), (SAMPLES, COUNTERS)), -6.0, 6.0)
    ordered = 0.5 * jnp.dot(mixing, sketch_rows) + jitter
    table = hosts_table(key)
    inverse = jnp.argsort(table, axis=1).astype(jnp.int32)
    shaped = ordered.reshape(SAMPLES, HOSTS // HOSTS_GRP, HOSTS_GRP, CNT)
    groups = jnp.arange(HOSTS // HOSTS_GRP, dtype=jnp.int32)[:, None]
    arrival = shaped[:, groups, inverse, :].reshape(SAMPLES, COUNTERS)
    return jnp.clip(arrival, -64.0, 64.0).astype(jnp.float32)


def setup_inputs(seed: int = 0) -> dict:
    splits = jax.random.split(jax.random.key(seed), 5)
    arrivals = draw_arrivals(jax.random.fold_in(splits[4], 71), 0)
    sketch = draw_sketch(jax.random.fold_in(splits[4], 71), 0)
    owner = draw_owner(jax.random.fold_in(splits[4], 71), 0)
    slot = jax.random.permutation(splits[3], SAMPLES).astype(jnp.int32)
    return {"arrivals": arrivals, "sketch": sketch, "owner": owner, "slot": slot}


highest = lax.Precision.HIGHEST

def product(former, latter):
    return jnp.dot(former.astype(jnp.float32), latter.astype(jnp.float32), precision=highest, preferred_element_type=jnp.float32)

def symmetric(matrix):
    return 0.5 * (matrix + matrix.T)

def lower_inverse(triangle):
    identity = jnp.eye(triangle.shape[0], dtype=jnp.float32)
    return jax.scipy.linalg.solve_triangular(triangle, identity, lower=True)

def orthonormal(columns):
    factor = jnp.linalg.cholesky(symmetric(product(columns.T, columns)))
    return jax.scipy.linalg.solve_triangular(factor, columns.T, lower=True).T

def shrink_factors(gram_matrix):
    subspace = orthonormal(gram_matrix[:, :ELL])
    reduced = symmetric(product(subspace.T, product(gram_matrix, subspace)))
    inverse_root = lower_inverse(jnp.linalg.cholesky(reduced))
    offset = 0.5 / jnp.sum(inverse_root * inverse_root)
    keeper = jnp.eye(ELL, dtype=jnp.float32) - offset * product(inverse_root.T, inverse_root)
    shrink_factor = jnp.linalg.cholesky(symmetric(keeper)).T
    return (product(shrink_factor, subspace.T), shrink_factor, reduced)

def reference(arrivals, sketch, owner, slot):
    shaped = arrivals.reshape(SAMPLES, N_GRP, HOSTS_GRP, CNT)
    groups = jnp.arange(N_GRP, dtype=jnp.int32)[:, None]
    placed = shaped[:, groups, owner.reshape(N_GRP, HOSTS_GRP), :].reshape(SAMPLES, COUNTERS)
    samples = placed[slot]
    first_batch = samples[:NEW]
    second_batch = samples[NEW:]
    stacked = jnp.concatenate([sketch, first_batch], axis=0)
    weights_one, factor_one, reduced_one = shrink_factors(product(stacked, stacked.T))
    middle = product(weights_one, stacked)
    stacked_two = jnp.concatenate([middle, second_batch], axis=0)
    weights_two, factor_two, reduced_two = shrink_factors(product(stacked_two, stacked_two.T))
    final_sketch = product(weights_two, stacked_two)
    spectrum = symmetric(product(factor_two, product(reduced_two, factor_two.T)))
    leading = orthonormal(spectrum[:, :TOP])
    directions = product(leading.T, final_sketch)
    small_gram = symmetric(product(leading.T, product(spectrum, leading)))
    inverse_root = lower_inverse(jnp.linalg.cholesky(small_gram))
    scores = product(samples, directions.T)
    coefficients = product(product(scores, inverse_root.T), inverse_root)
    residual = samples - product(coefficients, directions)
    return (final_sketch, residual)
```

```python
import jax
import jax.numpy as jnp
from jax import lax
from jax.experimental import pallas as pl
from jax.experimental.pallas import tpu as pltpu
from jax.sharding import Mesh
from jax.sharding import PartitionSpec as P

SUB = ("sub_0", "sub_1")
GRP_SUB = ("grp_0", "grp_1", "grp_2", "sub_0", "sub_1")
GRP = ("grp_0", "grp_1", "grp_2")

F32 = jnp.float32
HI = lax.Precision.HIGHEST
BLK = 32


def nn(a, b):
    return lax.dot_general(a, b, (((1,), (0,)), ((), ())), precision=HI, preferred_element_type=F32)


def nt(a, b):
    return lax.dot_general(a, b, (((1,), (1,)), ((), ())), precision=HI, preferred_element_type=F32)


def tn(a, b):
    return lax.dot_general(a, b, (((0,), (0,)), ((), ())), precision=HI, preferred_element_type=F32)


def iota(shape, axis):
    return lax.broadcasted_iota(jnp.int32, shape, axis)


def spread(tile, row):
    return jnp.broadcast_to(tile[row : row + 1], (8, 128))


def pivot_block(block, rows):
    groups = BLK // 8
    cols = []
    for j in range(BLK):
        cols.append([jnp.broadcast_to(block[8 * t : 8 * t + 8, j : j + 1], (8, 128)) if t >= j // 8 else None for t in range(groups)])
    sub = iota((8, 128), 0)
    width = len(rows[0])
    pivots = [None] * groups
    for k in range(BLK):
        tk, sk = divmod(k, 8)
        pivot = spread(cols[k][tk], sk)
        inverse = 1.0 / pivot
        scaled = [None] * groups
        for t in range(tk, groups):
            scaled[t] = cols[k][t] * inverse
        scaled[tk] = jnp.where(sub > sk, scaled[tk], 0.0)
        for j in range(k + 1, BLK):
            tj, sj = divmod(j, 8)
            element = spread(cols[k][tj], sj)
            for t in range(tj, groups):
                cols[j][t] = cols[j][t] - scaled[t] * element
        for c in range(width):
            row = spread(rows[tk][c], sk)
            for t in range(tk, groups):
                rows[t][c] = rows[t][c] - scaled[t] * row
        pivots[tk] = pivot if sk == 0 else jnp.where(sub == sk, pivot, pivots[tk])
    for t in range(groups):
        root = lax.rsqrt(pivots[t])
        for c in range(width):
            rows[t][c] = rows[t][c] * root
    return rows


def factor(work, width):
    tiles = width // 128

    def step(p, _):
        base = pl.multiple_of(p * BLK, BLK)
        lane = pl.multiple_of((p // 4) * 128, 128)
        block = work[pl.ds(base, BLK), pl.ds(lane, 128)]
        block = pltpu.roll(block, lax.rem(128 - (p % 4) * BLK, 128), 1)
        rows = [[work[pl.ds(base + 8 * t, 8), c * 128 : c * 128 + 128] for c in range(tiles)] for t in range(BLK // 8)]
        rows = pivot_block(block, rows)
        for t in range(BLK // 8):
            for c in range(tiles):
                work[pl.ds(base + 8 * t, 8), c * 128 : c * 128 + 128] = rows[t][c]

        panel = jnp.concatenate([jnp.concatenate(r, axis=1) for r in rows], axis=0)
        left = jnp.where(iota((BLK, 256), 1) >= base + BLK, panel[:, :256], 0.0)

        @pl.when(p < 3)
        def _():
            work[0:128, 0:width] = work[0:128, 0:width] - tn(left[:, :128], panel)

        @pl.when(p < 7)
        def _():
            work[128:256, 0:width] = work[128:256, 0:width] - tn(left[:, 128:], panel)
        return 0

    lax.fori_loop(0, 256 // BLK, step, 0)


def sym(x):
    return 0.5 * (x + x.T)


def shrink(yt, gram, work, yt_width):
    eye = (iota((256, 256), 0) == iota((256, 256), 1)).astype(F32)
    upper = iota((256, 256), 0) <= iota((256, 256), 1)
    work[:, 0:256] = nt(yt, yt)
    work[:, 256:640] = yt
    factor(work, 640)
    qt = work[:, 256:640]
    reduced = sym(nt(nn(qt, gram), qt))
    work[:, 0:256] = reduced
    work[:, 256:512] = eye
    factor(work, 512)
    root = work[:, 256:512]
    offset = 0.5 / jnp.sum(root * root, keepdims=True)
    work[:, 0:256] = eye - offset * tn(root, root)
    factor(work, 256)
    keeper = jnp.where(upper, work[:, 0:256], 0.0)
    return nn(keeper, qt), keeper, reduced


def small(matrix, right):
    tiles = right.shape[1] // 128
    rows = [[right[8 * t : 8 * t + 8, c * 128 : c * 128 + 128] for c in range(tiles)] for t in range(BLK // 8)]
    rows = pivot_block(matrix, rows)
    return jnp.concatenate([jnp.concatenate(r, axis=1) for r in rows], axis=0)


def chain_kernel(gram_ref, coef_ref, work, second_gram):
    lanes = iota((256, 384), 1)
    yt = jnp.where(lanes < 320, gram_ref[0:256, :], 0.0)
    inner = (iota((384, 384), 0) < 320) & (iota((384, 384), 1) < 320)
    second_gram[...] = jnp.where(inner, gram_ref[...], 0.0)
    weights, keeper, reduced = shrink(yt, second_gram[...], work, 640)
    corner = sym(nt(nn(keeper, reduced), keeper))
    mixed = nn(weights, gram_ref[...])
    side = mixed[:, 256:384]
    tail = gram_ref[256:384, 256:384]
    side = jnp.where(iota((256, 128), 1) < 64, pltpu.roll(side, 64, 1), 0.0)
    tail = pltpu.roll(tail, 64, 1)[64:128]
    tail = jnp.where(iota((64, 128), 1) < 64, tail, 0.0)
    second_gram[0:256, 0:256] = corner
    second_gram[0:256, 256:384] = side
    second_gram[256:384, 0:256] = side.T
    second_gram[256:320, 256:384] = tail
    second_gram[320:384, 256:384] = jnp.zeros((64, 128), F32)
    weights_two, keeper_two, reduced_two = shrink(second_gram[0:256, :], second_gram[...], work, 640)
    shifted = jnp.where(iota((256, 128), 1) >= 64, pltpu.roll(weights_two[:, 256:384], 64, 1), 0.0)
    whole = nn(weights_two[:, :256], weights)
    whole = jnp.concatenate([whole[:, :256], whole[:, 256:] + shifted], axis=1)
    coef_ref[0:256, :] = whole
    spectrum = sym(nt(nn(keeper_two, reduced_two), keeper_two))
    leading = spectrum[0:32, :]
    block = nt(leading, jnp.concatenate([leading, jnp.zeros((96, 256), F32)], axis=0))
    ut = small(block, leading)
    padded = jnp.concatenate([ut, jnp.zeros((96, 256), F32)], axis=0)
    block = nt(nn(ut, spectrum), padded)
    block = 0.5 * (block + nt(ut, jnp.concatenate([nn(ut, spectrum), jnp.zeros((96, 256), F32)], axis=0)))
    towards = nn(ut, whole)
    scores = nn(towards, gram_ref[...])[:, 256:384]
    both = small(block, jnp.concatenate([towards, scores], axis=1))
    ident = (iota((128, 384), 1) == iota((128, 384), 0) + 256).astype(F32)
    coef_ref[256:384, :] = ident - tn(both[:, 384:512], both[:, :384])


def chain(gram):
    return pl.pallas_call(
        chain_kernel,
        out_shape=jax.ShapeDtypeStruct((384, 384), F32),
        in_specs=[pl.BlockSpec(memory_space=pltpu.VMEM)],
        out_specs=pl.BlockSpec(memory_space=pltpu.VMEM),
        scratch_shapes=[pltpu.VMEM((256, 640), F32), pltpu.VMEM((384, 384), F32)],
    )(gram)


def local(arrivals, sketch, owner, slot):
    arrived_rows, arrived_columns = arrivals.shape
    host_count = owner.shape[0]
    shaped = arrivals.reshape(arrived_rows, host_count, arrived_columns // host_count)
    placed = jnp.take(shaped, owner, axis=1).reshape(arrived_rows, arrived_columns)
    regrouped = lax.all_to_all(placed, SUB, split_axis=1, concat_axis=0, tiled=True)
    samples = jnp.take(regrouped, slot, axis=0)
    stacked = jnp.concatenate([sketch, samples], axis=0)
    gram = lax.psum(nt(stacked, stacked), GRP_SUB)
    outs = nn(chain(gram), stacked)
    return (outs[:256], outs[256:])


def solution(mesh):
    split = Mesh(mesh.devices.reshape(2, 4, 2, 2, 8), ("grp_0", "grp_1", "grp_2", "sub_0", "sub_1"))
    placed = (P(SUB, GRP), P(None, GRP_SUB), P(GRP), P())
    return jax.shard_map(
        local,
        mesh=split,
        in_specs=placed,
        out_specs=(P(None, GRP_SUB), P(None, GRP_SUB)),
        check_vma=False,
    )
```

```python
import jax
import jax.numpy as jnp
from jax import lax
from jax.experimental import pallas as pl
from jax.experimental.pallas import tpu as pltpu
from jax.sharding import Mesh
from jax.sharding import PartitionSpec as P

SUB = ("sub_0", "sub_1")
GRP_SUB = ("grp_0", "grp_1", "grp_2", "sub_0", "sub_1")
GRP = ("grp_0", "grp_1", "grp_2")

F32 = jnp.float32
HI = lax.Precision.HIGHEST
BLK = 32


def nn(a, b):
    return lax.dot_general(a, b, (((1,), (0,)), ((), ())), precision=HI, preferred_element_type=F32)


def nt(a, b):
    return lax.dot_general(a, b, (((1,), (1,)), ((), ())), precision=HI, preferred_element_type=F32)


def tn(a, b):
    return lax.dot_general(a, b, (((0,), (0,)), ((), ())), precision=HI, preferred_element_type=F32)


def iota(shape, axis):
    return lax.broadcasted_iota(jnp.int32, shape, axis)


def spread(tile, row):
    return jnp.broadcast_to(tile[row : row + 1], (8, 128))


def pivot_block(block, rows):
    groups = BLK // 8
    cols = []
    for j in range(BLK):
        cols.append([jnp.broadcast_to(block[8 * t : 8 * t + 8, j : j + 1], (8, 128)) if t >= j // 8 else None for t in range(groups)])
    sub = iota((8, 128), 0)
    width = len(rows[0])
    pivots = [None] * groups
    for k in range(BLK):
        tk, sk = divmod(k, 8)
        pivot = spread(cols[k][tk], sk)
        inverse = 1.0 / pivot
        scaled = [None] * groups
        for t in range(tk, groups):
            scaled[t] = cols[k][t] * inverse
        scaled[tk] = jnp.where(sub > sk, scaled[tk], 0.0)
        for j in range(k + 1, BLK):
            tj, sj = divmod(j, 8)
            element = spread(cols[k][tj], sj)
            for t in range(tj, groups):
                cols[j][t] = cols[j][t] - scaled[t] * element
        for c in range(width):
            row = spread(rows[tk][c], sk)
            for t in range(tk, groups):
                rows[t][c] = rows[t][c] - scaled[t] * row
        pivots[tk] = pivot if sk == 0 else jnp.where(sub == sk, pivot, pivots[tk])
    for t in range(groups):
        root = lax.rsqrt(pivots[t])
        for c in range(width):
            rows[t][c] = rows[t][c] * root
    return rows


def factor(work, width):
    tiles = width // 128

    def step(p, _):
        base = pl.multiple_of(p * BLK, BLK)
        lane = pl.multiple_of((p // 4) * 128, 128)
        block = work[pl.ds(base, BLK), pl.ds(lane, 128)]
        block = pltpu.roll(block, lax.rem(128 - (p % 4) * BLK, 128), 1)
        rows = [[work[pl.ds(base + 8 * t, 8), c * 128 : c * 128 + 128] for c in range(tiles)] for t in range(BLK // 8)]
        rows = pivot_block(block, rows)
        for t in range(BLK // 8):
            for c in range(tiles):
                work[pl.ds(base + 8 * t, 8), c * 128 : c * 128 + 128] = rows[t][c]

        panel = jnp.concatenate([jnp.concatenate(r, axis=1) for r in rows], axis=0)
        left = jnp.where(iota((BLK, 256), 1) >= base + BLK, panel[:, :256], 0.0)

        @pl.when(p < 3)
        def _():
            work[0:128, 0:width] = work[0:128, 0:width] - tn(left[:, :128], panel)

        @pl.when(p < 7)
        def _():
            work[128:256, 0:width] = work[128:256, 0:width] - tn(left[:, 128:], panel)
        return 0

    lax.fori_loop(0, 256 // BLK, step, 0)


def sym(x):
    return 0.5 * (x + x.T)


def shrink(yt, gram, work, yt_width):
    eye = (iota((256, 256), 0) == iota((256, 256), 1)).astype(F32)
    upper = iota((256, 256), 0) <= iota((256, 256), 1)
    work[:, 0:256] = nt(yt, yt)
    work[:, 256:640] = yt
    factor(work, 640)
    qt = work[:, 256:640]
    reduced = sym(nt(nn(qt, gram), qt))
    work[:, 0:256] = reduced
    work[:, 256:512] = eye
    factor(work, 512)
    root = work[:, 256:512]
    offset = 0.5 / jnp.sum(root * root, keepdims=True)
    work[:, 0:256] = eye - offset * tn(root, root)
    factor(work, 256)
    keeper = jnp.where(upper, work[:, 0:256], 0.0)
    return nn(keeper, qt), keeper, reduced


def small(matrix, right):
    tiles = right.shape[1] // 128
    rows = [[right[8 * t : 8 * t + 8, c * 128 : c * 128 + 128] for c in range(tiles)] for t in range(BLK // 8)]
    rows = pivot_block(matrix, rows)
    return jnp.concatenate([jnp.concatenate(r, axis=1) for r in rows], axis=0)


def chain_kernel(packed_ref, sketch_ref, samples_ref, final_ref, residual_ref, work, gram_ref, second_gram, coef_ref):
    index = 0
    for i in range(3):
        for j in range(i + 1):
            tile = packed_ref[index * 128 : index * 128 + 128, :]
            gram_ref[i * 128 : i * 128 + 128, j * 128 : j * 128 + 128] = tile
            if i != j:
                gram_ref[j * 128 : j * 128 + 128, i * 128 : i * 128 + 128] = tile.T
            index += 1
    lanes = iota((256, 384), 1)
    yt = jnp.where(lanes < 320, gram_ref[0:256, :], 0.0)
    inner = (iota((384, 384), 0) < 320) & (iota((384, 384), 1) < 320)
    second_gram[...] = jnp.where(inner, gram_ref[...], 0.0)
    weights, keeper, reduced = shrink(yt, second_gram[...], work, 640)
    corner = sym(nt(nn(keeper, reduced), keeper))
    mixed = nn(weights, gram_ref[...])
    side = mixed[:, 256:384]
    tail = gram_ref[256:384, 256:384]
    side = jnp.where(iota((256, 128), 1) < 64, pltpu.roll(side, 64, 1), 0.0)
    tail = pltpu.roll(tail, 64, 1)[64:128]
    tail = jnp.where(iota((64, 128), 1) < 64, tail, 0.0)
    second_gram[0:256, 0:256] = corner
    second_gram[0:256, 256:384] = side
    second_gram[256:384, 0:256] = side.T
    second_gram[256:320, 256:384] = tail
    second_gram[320:384, 256:384] = jnp.zeros((64, 128), F32)
    weights_two, keeper_two, reduced_two = shrink(second_gram[0:256, :], second_gram[...], work, 640)
    shifted = jnp.where(iota((256, 128), 1) >= 64, pltpu.roll(weights_two[:, 256:384], 64, 1), 0.0)
    whole = nn(weights_two[:, :256], weights)
    whole = jnp.concatenate([whole[:, :256], whole[:, 256:] + shifted], axis=1)
    coef_ref[0:256, :] = whole
    spectrum = sym(nt(nn(keeper_two, reduced_two), keeper_two))
    leading = spectrum[0:32, :]
    block = nt(leading, jnp.concatenate([leading, jnp.zeros((96, 256), F32)], axis=0))
    ut = small(block, leading)
    padded = jnp.concatenate([ut, jnp.zeros((96, 256), F32)], axis=0)
    block = nt(nn(ut, spectrum), padded)
    block = 0.5 * (block + nt(ut, jnp.concatenate([nn(ut, spectrum), jnp.zeros((96, 256), F32)], axis=0)))
    towards = nn(ut, whole)
    scores = nn(towards, gram_ref[...])[:, 256:384]
    both = small(block, jnp.concatenate([towards, scores], axis=1))
    ident = (iota((128, 384), 1) == iota((128, 384), 0) + 256).astype(F32)
    coef_ref[256:384, :] = ident - tn(both[:, 384:512], both[:, :384])


    def columns(i, _):
        at = pl.ds(pl.multiple_of(i * 256, 256), 256)
        both = nn(coef_ref[:, 0:256], sketch_ref[:, at]) + nn(coef_ref[:, 256:384], samples_ref[:, at])
        final_ref[:, at] = both[:256]
        residual_ref[:, at] = both[256:]
        return 0

    lax.fori_loop(0, 4, columns, 0)


def chain(packed, sketch, samples):
    vmem = pl.BlockSpec(memory_space=pltpu.VMEM)
    return pl.pallas_call(
        chain_kernel,
        out_shape=(jax.ShapeDtypeStruct((256, 1024), F32), jax.ShapeDtypeStruct((128, 1024), F32)),
        in_specs=[vmem] * 3,
        out_specs=(vmem, vmem),
        scratch_shapes=[pltpu.VMEM((256, 640), F32), pltpu.VMEM((384, 384), F32), pltpu.VMEM((384, 384), F32), pltpu.VMEM((384, 384), F32)],
    )(packed, sketch, samples)


def gram_kernel(slot_ref, sketch_ref, landed_ref, packed_ref, samples_ref):
    pick = (iota((128, 128), 0) == slot_ref[...]).astype(F32)
    samples_ref[...] = tn(pick, landed_ref[...])
    packed_ref[0:128, :] = nt(sketch_ref[0:128, :], sketch_ref[0:128, :])
    packed_ref[128:256, :] = nt(sketch_ref[128:256, :], sketch_ref[0:128, :])
    packed_ref[256:384, :] = nt(sketch_ref[128:256, :], sketch_ref[128:256, :])
    packed_ref[384:512, :] = nt(samples_ref[...], sketch_ref[0:128, :])
    packed_ref[512:640, :] = nt(samples_ref[...], sketch_ref[128:256, :])
    packed_ref[640:768, :] = nt(samples_ref[...], samples_ref[...])


def gram_terms(slot, sketch, landed):
    vmem = pl.BlockSpec(memory_space=pltpu.VMEM)
    return pl.pallas_call(
        gram_kernel,
        out_shape=(jax.ShapeDtypeStruct((768, 128), F32), jax.ShapeDtypeStruct((128, 1024), F32)),
        in_specs=[vmem] * 3,
        out_specs=(vmem, vmem),
    )(slot, sketch, landed)


def place_kernel(owner_ref, arrivals_ref, out_ref):
    quarter = lax.broadcasted_iota(jnp.int32, (8, 128), 1) // 32

    def step(v, _):
        pieces = []
        for i in range(4):
            host = owner_ref[v * 4 + i]
            tile = arrivals_ref[:, pl.ds(pl.multiple_of((host // 4) * 128, 128), 128)]
            pieces.append(pltpu.roll(tile, lax.rem(i * 32 - lax.rem(host, 4) * 32 + 128, 128), 1))
        tile = jnp.where(quarter == 0, pieces[0], jnp.where(quarter == 1, pieces[1], jnp.where(quarter == 2, pieces[2], pieces[3])))
        out_ref[v // 8, :, pl.ds(pl.multiple_of(lax.rem(v, 8) * 128, 128), 128)] = tile
        return 0

    lax.fori_loop(0, 128, step, 0, unroll=16)


def place(owner, arrivals):
    return pl.pallas_call(
        place_kernel,
        out_shape=jax.ShapeDtypeStruct((16, 8, 1024), F32),
        in_specs=[pl.BlockSpec(memory_space=pltpu.SMEM), pl.BlockSpec(memory_space=pltpu.VMEM)],
        out_specs=pl.BlockSpec(memory_space=pltpu.VMEM),
    )(owner, arrivals)


MESH = pl.DeviceIdType.MESH


def spot():
    return tuple(lax.axis_index(name) for name in GRP_SUB)


def exchange_kernel(placed_ref, out_ref, landed, send_sems, recv_sems, own_sem):
    y_hi, x, core, y_lo, z = spot()
    me = y_lo * 8 + z

    def device(j):
        return (y_hi, x, core, j // 8, lax.rem(j, 8))

    barrier = pltpu.get_barrier_semaphore()
    for s in range(1, 16):
        pl.semaphore_signal(barrier, inc=1, device_id=device(lax.rem(me + s, 16)), device_id_type=MESH)
    own = pltpu.make_async_copy(placed_ref.at[me], landed.at[me], own_sem)
    own.start()
    pl.semaphore_wait(barrier, 15)
    copies = []
    for s in (8, 4, 12, 3, 5, 11, 13, 2, 6, 10, 14, 1, 7, 9, 15):
        peer = lax.rem(me + s, 16)
        copy = pltpu.make_async_remote_copy(
            src_ref=placed_ref.at[peer], dst_ref=landed.at[me],
            send_sem=send_sems.at[s], recv_sem=recv_sems.at[s],
            device_id=device(peer), device_id_type=MESH)
        copy.start()
        copies.append(copy)
    own.wait()
    for copy in copies:
        copy.wait_recv()
    out_ref[...] = landed[...]
    for copy in copies:
        copy.wait_send()


def exchange(placed):
    return pl.pallas_call(
        exchange_kernel,
        out_shape=jax.ShapeDtypeStruct((16, 8, 1024), F32),
        in_specs=[pl.BlockSpec(memory_space=pltpu.VMEM)],
        out_specs=pl.BlockSpec(memory_space=pltpu.VMEM),
        scratch_shapes=[pltpu.VMEM((16, 8, 1024), F32), pltpu.SemaphoreType.DMA((16,)), pltpu.SemaphoreType.DMA((16,)), pltpu.SemaphoreType.DMA],
        compiler_params=pltpu.CompilerParams(collective_id=0, has_side_effects=True),
    )(placed)


def reduce_kernel(part_ref, out_ref, twin, half, plane, piece, column, share, whole,
                  twin_sems, plane_send, plane_recv, column_send, column_recv, share_send, share_recv, back_send, back_recv):
    y_hi, x, core, y_lo, z = spot()
    me = (y_hi * 2 + y_lo) * 4 + x

    def in_plane(q):
        y = q // 4
        return (y // 2, lax.rem(q, 4), core, lax.rem(y, 2), z)

    def in_column(k):
        return (y_hi, x, core, y_lo, k)

    other = (y_hi, x, 1 - core, y_lo, z)
    barrier = pltpu.get_barrier_semaphore()
    pl.semaphore_signal(barrier, inc=1, device_id=other, device_id_type=MESH)
    for s in range(1, 16):
        pl.semaphore_signal(barrier, inc=1, device_id=in_plane(lax.rem(me + s, 16)), device_id_type=MESH)
    for s in range(1, 8):
        pl.semaphore_signal(barrier, inc=1, device_id=in_column(lax.rem(z + s, 8)), device_id_type=MESH)
    pl.semaphore_wait(barrier, 23)

    def send(source, target, send_sem, recv_sem, device):
        copy = pltpu.make_async_remote_copy(src_ref=source, dst_ref=target, send_sem=send_sem, recv_sem=recv_sem, device_id=device, device_id_type=MESH)
        copy.start()
        return copy

    first = send(part_ref.at[1 - core], twin, twin_sems.at[0], twin_sems.at[1], other)
    first.wait_recv()
    half[...] = part_ref[core] + twin[...]

    scattered = []
    for s in range(1, 16):
        peer = lax.rem(me + s, 16)
        scattered.append(send(half.at[peer], plane.at[s], plane_send.at[s], plane_recv.at[s], in_plane(peer)))
    total = half[me]
    for s in range(1, 16):
        scattered[s - 1].wait_recv()
        total = total + plane[s]
    piece[...] = total

    spread_out = []
    for s in range(1, 8):
        peer = lax.rem(z + s, 8)
        spread_out.append(send(piece, column.at[z], column_send.at[s], column_recv.at[s], in_column(peer)))
    column[z] = piece[...]
    for copy in spread_out:
        copy.wait_recv()
    total = column[0]
    for k in range(1, 8):
        total = total + column[k]
    share[...] = total

    gathered = []
    for s in range(1, 16):
        peer = lax.rem(me + s, 16)
        gathered.append(send(share, whole.at[core, me], share_send.at[s], share_recv.at[s], in_plane(peer)))
    whole[core, me] = share[...]
    back = [send(share, whole.at[core, me], back_send.at[0], back_recv.at[0], other)]
    for s in range(1, 16):
        gathered[s - 1].wait_recv()
        source = lax.rem(me + 16 - s, 16)
        back.append(send(whole.at[core, source], whole.at[core, source], back_send.at[s], back_recv.at[s], other))
    for copy in back:
        copy.wait_recv()
    out_ref[...] = whole[...]
    for copy in [first] + scattered + spread_out + gathered + back:
        copy.wait_send()


def reduce_all(part):
    dma = pltpu.SemaphoreType.DMA
    return pl.pallas_call(
        reduce_kernel,
        out_shape=jax.ShapeDtypeStruct((2, 16, 24, 128), F32),
        in_specs=[pl.BlockSpec(memory_space=pltpu.VMEM)],
        out_specs=pl.BlockSpec(memory_space=pltpu.VMEM),
        scratch_shapes=[
            pltpu.VMEM((16, 24, 128), F32), pltpu.VMEM((16, 24, 128), F32), pltpu.VMEM((16, 24, 128), F32),
            pltpu.VMEM((24, 128), F32), pltpu.VMEM((8, 24, 128), F32), pltpu.VMEM((24, 128), F32), pltpu.VMEM((2, 16, 24, 128), F32),
            dma((2,)), dma((16,)), dma((16,)), dma((8,)), dma((8,)), dma((16,)), dma((16,)), dma((16,)), dma((16,)),
        ],
        compiler_params=pltpu.CompilerParams(collective_id=1, has_side_effects=True),
    )(part)


def local(arrivals, sketch, owner, slot):
    landed = exchange(place(owner, arrivals)).reshape(128, 1024)
    packed, samples = gram_terms(slot.reshape(1, 128), sketch, landed)
    total = reduce_all(packed.reshape(2, 16, 24, 128)).reshape(768, 128)
    return chain(total, sketch, samples)


def solution(mesh):
    split = Mesh(mesh.devices.reshape(2, 4, 2, 2, 8), ("grp_0", "grp_1", "grp_2", "sub_0", "sub_1"))
    placed = (P(SUB, GRP), P(None, GRP_SUB), P(GRP), P())
    return jax.shard_map(
        local,
        mesh=split,
        in_specs=placed,
        out_specs=(P(None, GRP_SUB), P(None, GRP_SUB)),
        check_vma=False,
    )
```

```python
import jax
import jax.numpy as jnp
from jax import lax
from jax.experimental import pallas as pl
from jax.experimental.pallas import tpu as pltpu
from jax.sharding import Mesh
from jax.sharding import PartitionSpec as P

SUB = ("sub_0", "sub_1")
GRP_SUB = ("grp_0", "grp_1", "grp_2", "sub_0", "sub_1")
GRP = ("grp_0", "grp_1", "grp_2")
MESH = pl.DeviceIdType.MESH

F32 = jnp.float32
HI = lax.Precision.HIGHEST
BLK = 32


def nn(a, b):
    return lax.dot_general(a, b, (((1,), (0,)), ((), ())), precision=HI, preferred_element_type=F32)


def nt(a, b):
    return lax.dot_general(a, b, (((1,), (1,)), ((), ())), precision=HI, preferred_element_type=F32)


def tn(a, b):
    return lax.dot_general(a, b, (((0,), (0,)), ((), ())), precision=HI, preferred_element_type=F32)


def iota(shape, axis):
    return lax.broadcasted_iota(jnp.int32, shape, axis)


def spread(tile, row):
    return jnp.broadcast_to(tile[row : row + 1], (8, 128))


def pivot_block(cols, rows):
    groups = BLK // 8
    sub = iota((8, 128), 0)
    width = len(rows[0])
    roots = [None] * groups
    pivot = spread(cols[0][0], 0)
    for k in range(BLK):
        tk, sk = divmod(k, 8)
        root = lax.rsqrt(pivot)
        inverse = root * root
        if k + 1 < BLK:
            tj, sj = divmod(k + 1, 8)
            element = spread(cols[k][tj], sj)
            pivot = spread(cols[k + 1][tj], sj) - (element * element) * inverse
        scaled = [None] * groups
        for t in range(tk, groups):
            scaled[t] = cols[k][t] * inverse
        scaled[tk] = jnp.where(sub > sk, scaled[tk], 0.0)
        for j in range(k + 1, BLK):
            tj, sj = divmod(j, 8)
            element = spread(cols[k][tj], sj)
            for t in range(tj, groups):
                cols[j][t] = cols[j][t] - scaled[t] * element
        for c in range(width):
            row = spread(rows[tk][c], sk)
            for t in range(tk, groups):
                rows[t][c] = rows[t][c] - scaled[t] * row
        roots[tk] = root if sk == 0 else jnp.where(sub == sk, root, roots[tk])
    for t in range(groups - 1):
        roots[t] = jnp.minimum(roots[t], roots[t] + roots[groups - 1])
    return [[tile * roots[t] for tile in rows[t]] for t in range(groups)]


def columns_of(tiles, offset):
    cols = []
    for j in range(BLK):
        lane = jnp.full((8, 128), j, jnp.int32) + offset
        cols.append([jnp.take_along_axis(tiles[t], lane, axis=1) if t >= j // 8 else None for t in range(BLK // 8)])
    return cols


def join(rows):
    return jnp.concatenate([jnp.concatenate(r, axis=1) for r in rows], axis=0)


def factor(work, last, turned, early, late):
    groups = BLK // 8

    def step(p, low, first, end):
        base = pl.multiple_of(p * BLK, BLK)
        lane = pl.multiple_of((p // 4) * 128, 128)
        span = slice(first * 128, end * 128)
        block = [work[pl.ds(base + 8 * t, 8), pl.ds(lane, 128)] for t in range(groups)]
        rows = [[work[pl.ds(base + 8 * t, 8), c * 128 : c * 128 + 128] for c in range(first, end)] for t in range(groups)]
        cols = columns_of(block, lax.rem(p, 4) * BLK)
        left = jnp.where(iota((256 - low, 128), 0) >= base + BLK - low, turned[low:, :], 0.0)[:, :BLK]
        work[low:, span] = work[low:, span] - nn(left, last[:, span])
        rows = pivot_block(cols, rows)
        for t in range(groups):
            for c in range(first, end):
                work[pl.ds(base + 8 * t, 8), c * 128 : c * 128 + 128] = rows[t][c - first]
        panel = join(rows)
        last[:, span] = panel
        turned[low:, 0:BLK] = panel[:, low - first * 128 : 256 - first * 128].T

        @pl.when(p < 7)
        def _():
            below = pl.ds(base + BLK, BLK)
            work[below, span] = work[below, span] - nn(turned[below, 0:BLK], panel)
        return 0

    last[...] = jnp.zeros_like(last)
    turned[...] = jnp.zeros_like(turned)
    lax.fori_loop(0, 4, lambda p, _: step(p, 0, *early), 0)
    lax.fori_loop(4, 8, lambda p, _: step(p, 128, *late), 0)


def near_identity_root(excess):
    down, across = iota((256, 256), 0), iota((256, 256), 1)
    half = jnp.where(down > across, 1.0, jnp.where(down == across, 0.5, 0.0)).astype(F32)

    def onward(x):
        return -half * (excess + nt(x, x))

    def more(state):
        return (state[1] > 1e-11) & (state[2] < 64)

    def body(state):
        x = onward(state[0])
        y = onward(x)
        return y, jnp.sum((y - x) * (y - x)), state[2] + 1

    return lax.while_loop(more, body, (-half * excess, jnp.float32(1.0), jnp.int32(0)))[0]


def sym(x):
    return 0.5 * (x + x.T)


def shrink(yt, gram, work, last, turned):
    eye = (iota((256, 256), 0) == iota((256, 256), 1)).astype(F32)
    work[:, 0:256] = nt(yt, yt)
    work[:, 256:640] = yt
    factor(work, last, turned, (0, 5), (1, 5))
    qt = work[:, 256:640]
    reduced = sym(nt(nn(qt, gram), qt))
    work[:, 0:256] = reduced
    work[:, 256:512] = eye
    factor(work, last, turned, (0, 3), (1, 4))
    root = work[:, 256:512]
    offset = 0.5 / jnp.sum(root * root, keepdims=True)
    keeper = eye + near_identity_root(offset * tn(root, root)).T
    return nn(keeper, qt), keeper, reduced


def small(matrix, right):
    tiles = right.shape[1] // 128
    groups = BLK // 8
    rows = [[right[8 * t : 8 * t + 8, c * 128 : c * 128 + 128] for c in range(tiles)] for t in range(groups)]
    return join(pivot_block(columns_of([matrix[8 * t : 8 * t + 8] for t in range(groups)], 0), rows))


def chain_kernel(packed_ref, sketch_ref, samples_ref, final_ref, residual_ref, work, last, turned, gram_ref, second_gram, coef_ref):
    index = 0
    for i in range(3):
        for j in range(i + 1):
            tile = packed_ref[index * 128 : index * 128 + 128, :]
            gram_ref[i * 128 : i * 128 + 128, j * 128 : j * 128 + 128] = tile
            if i != j:
                gram_ref[j * 128 : j * 128 + 128, i * 128 : i * 128 + 128] = tile.T
            index += 1
    lanes = iota((256, 384), 1)
    yt = jnp.where(lanes < 320, gram_ref[0:256, :], 0.0)
    inner = (iota((384, 384), 0) < 320) & (iota((384, 384), 1) < 320)
    second_gram[...] = jnp.where(inner, gram_ref[...], 0.0)
    weights, keeper, reduced = shrink(yt, second_gram[...], work, last, turned)
    corner = sym(nt(nn(keeper, reduced), keeper))
    mixed = nn(weights, gram_ref[...])
    side = mixed[:, 256:384]
    tail = gram_ref[256:384, 256:384]
    side = jnp.where(iota((256, 128), 1) < 64, pltpu.roll(side, 64, 1), 0.0)
    tail = pltpu.roll(tail, 64, 1)[64:128]
    tail = jnp.where(iota((64, 128), 1) < 64, tail, 0.0)
    second_gram[0:256, 0:256] = corner
    second_gram[0:256, 256:384] = side
    second_gram[256:384, 0:256] = side.T
    second_gram[256:320, 256:384] = tail
    second_gram[320:384, 256:384] = jnp.zeros((64, 128), F32)
    weights_two, keeper_two, reduced_two = shrink(second_gram[0:256, :], second_gram[...], work, last, turned)
    shifted = jnp.where(iota((256, 128), 1) >= 64, pltpu.roll(weights_two[:, 256:384], 64, 1), 0.0)
    whole = nn(weights_two[:, :256], weights)
    whole = jnp.concatenate([whole[:, :256], whole[:, 256:] + shifted], axis=1)
    coef_ref[0:256, :] = whole
    spectrum = sym(nt(nn(keeper_two, reduced_two), keeper_two))
    leading = spectrum[0:32, :]
    block = nt(leading, jnp.concatenate([leading, jnp.zeros((96, 256), F32)], axis=0))
    ut = small(block, leading)
    padded = jnp.concatenate([ut, jnp.zeros((96, 256), F32)], axis=0)
    block = nt(nn(ut, spectrum), padded)
    block = 0.5 * (block + nt(ut, jnp.concatenate([nn(ut, spectrum), jnp.zeros((96, 256), F32)], axis=0)))
    towards = nn(ut, whole)
    scores = nn(towards, gram_ref[...])[:, 256:384]
    both = small(block, jnp.concatenate([towards, scores], axis=1))
    ident = (iota((128, 384), 1) == iota((128, 384), 0) + 256).astype(F32)
    coef_ref[256:384, :] = ident - tn(both[:, 384:512], both[:, :384])


    def columns(i, _):
        at = pl.ds(pl.multiple_of(i * 256, 256), 256)
        both = nn(coef_ref[:, 0:256], sketch_ref[:, at]) + nn(coef_ref[:, 256:384], samples_ref[:, at])
        final_ref[:, at] = both[:256]
        residual_ref[:, at] = both[256:]
        return 0

    lax.fori_loop(0, 4, columns, 0)


def chain(packed, sketch, samples):
    vmem = pl.BlockSpec(memory_space=pltpu.VMEM)
    square = pltpu.VMEM((384, 384), F32)
    return pl.pallas_call(
        chain_kernel,
        out_shape=(jax.ShapeDtypeStruct((256, 1024), F32), jax.ShapeDtypeStruct((128, 1024), F32)),
        in_specs=[vmem] * 3,
        out_specs=(vmem, vmem),
        scratch_shapes=[pltpu.VMEM((256, 640), F32), pltpu.VMEM((BLK, 640), F32), pltpu.VMEM((256, 128), F32), square, square, square],
    )(packed, sketch, samples)


def spot():
    return tuple(lax.axis_index(name) for name in GRP_SUB)


def place_tile(owner_ref, arrivals_ref, at):
    quarter = iota((8, 128), 1) // 32
    tile = None
    for i in range(4):
        host = owner_ref[at + i]
        source = arrivals_ref[:, pl.ds(pl.multiple_of((host >> 2) * 128, 128), 128)]
        turned = pltpu.roll(source, ((i - host) & 3) * 32, 1)
        tile = turned if i == 0 else jnp.where(quarter == i, turned, tile)
    return tile


def place_kernel(owner_ref, arrivals_ref, placed_ref):
    def block(j, _):
        for v in range(8):
            placed_ref[j, :, v * 128 : v * 128 + 128] = place_tile(owner_ref, arrivals_ref, j * 32 + v * 4)
        return 0

    lax.fori_loop(0, 16, block, 0)


def place(owner, arrivals):
    return pl.pallas_call(
        place_kernel,
        out_shape=jax.ShapeDtypeStruct((16, 8, 1024), F32),
        in_specs=[pl.BlockSpec(memory_space=pltpu.SMEM), pl.BlockSpec(memory_space=pltpu.VMEM)],
        out_specs=pl.BlockSpec(memory_space=pltpu.VMEM),
    )(owner, arrivals)


def collect_kernel(slot_ref, placed, sketch_ref, total_ref, samples_ref,
                   landed, part, twin, half, plane, piece, column, share, whole,
                   move_send, move_recv, twin_sems, plane_send, plane_recv, column_send, column_recv, share_send, share_recv, back_send, back_recv):
    y_hi, x, core, y_lo, z = spot()
    me_sub = y_lo * 8 + z
    me = (y_hi * 2 + y_lo) * 4 + x

    def in_sub(j):
        return (y_hi, x, core, j // 8, lax.rem(j, 8))

    def in_plane(q):
        y = q // 4
        return (y // 2, lax.rem(q, 4), core, lax.rem(y, 2), z)

    def in_column(k):
        return (y_hi, x, core, y_lo, k)

    other = (y_hi, x, 1 - core, y_lo, z)

    def send(source, target, send_sem, recv_sem, device):
        copy = pltpu.make_async_remote_copy(src_ref=source, dst_ref=target, send_sem=send_sem, recv_sem=recv_sem, device_id=device, device_id_type=MESH)
        copy.start()
        return copy

    barrier = pltpu.get_barrier_semaphore()
    pl.semaphore_signal(barrier, inc=1, device_id=other, device_id_type=MESH)
    for s in range(1, 16):
        pl.semaphore_signal(barrier, inc=1, device_id=in_sub(lax.rem(me_sub + s, 16)), device_id_type=MESH)
        pl.semaphore_signal(barrier, inc=1, device_id=in_plane(lax.rem(me + s, 16)), device_id_type=MESH)

    landed[me_sub] = placed[me_sub]
    pl.semaphore_wait(barrier, 31)
    moves = []
    for s in (8, 4, 12, 3, 5, 11, 13, 2, 6, 10, 14, 1, 7, 9, 15):
        peer = lax.rem(me_sub + s, 16)
        moves.append(send(placed.at[peer], landed.at[me_sub], move_send.at[s], move_recv.at[s], in_sub(peer)))

    def put(index, block):
        rows = block.reshape(16, 8, 128)
        for r in range(16):
            at = index * 16 + r
            part[at // 48, (at % 48) // 3, (at % 3) * 8 : (at % 3) * 8 + 8, :] = rows[r]

    put(0, nt(sketch_ref[0:128, :], sketch_ref[0:128, :]))
    put(1, nt(sketch_ref[128:256, :], sketch_ref[0:128, :]))
    put(2, nt(sketch_ref[128:256, :], sketch_ref[128:256, :]))
    for copy in moves:
        copy.wait_recv()
    pick = (iota((128, 128), 0) == slot_ref[...]).astype(F32)
    samples_ref[...] = tn(pick, landed[...].reshape(128, 1024))
    put(3, nt(samples_ref[...], sketch_ref[0:128, :]))
    put(4, nt(samples_ref[...], sketch_ref[128:256, :]))
    put(5, nt(samples_ref[...], samples_ref[...]))

    first = send(part.at[1 - core], twin, twin_sems.at[0], twin_sems.at[1], other)
    first.wait_recv()
    half[...] = part[core] + twin[...]

    scattered = []
    for s in range(1, 16):
        peer = lax.rem(me + s, 16)
        scattered.append(send(half.at[peer], plane.at[s], plane_send.at[s], plane_recv.at[s], in_plane(peer)))
    total = half[me]
    for s in range(1, 16):
        scattered[s - 1].wait_recv()
        total = total + plane[s]
    piece[...] = total

    spread_out = []
    for s in range(1, 8):
        peer = lax.rem(z + s, 8)
        spread_out.append(send(piece, column.at[z], column_send.at[s], column_recv.at[s], in_column(peer)))
    column[z] = piece[...]
    for copy in spread_out:
        copy.wait_recv()
    total = column[0]
    for k in range(1, 8):
        total = total + column[k]
    share[...] = total

    gathered = []
    for s in range(1, 16):
        peer = lax.rem(me + s, 16)
        gathered.append(send(share, whole.at[core, me], share_send.at[s], share_recv.at[s], in_plane(peer)))
    whole[core, me] = share[...]
    back = [send(share, whole.at[core, me], back_send.at[0], back_recv.at[0], other)]
    for s in range(1, 16):
        gathered[s - 1].wait_recv()
        source = lax.rem(me + 16 - s, 16)
        back.append(send(whole.at[core, source], whole.at[core, source], back_send.at[s], back_recv.at[s], other))
    for copy in back:
        copy.wait_recv()
    total_ref[...] = whole[...].reshape(768, 128)
    for copy in moves + [first] + scattered + spread_out + gathered + back:
        copy.wait_send()


def collect(owner, slot, arrivals, sketch):
    dma = pltpu.SemaphoreType.DMA
    vmem = pl.BlockSpec(memory_space=pltpu.VMEM)
    return pl.pallas_call(
        collect_kernel,
        out_shape=(jax.ShapeDtypeStruct((768, 128), F32), jax.ShapeDtypeStruct((128, 1024), F32)),
        in_specs=[vmem, vmem, vmem],
        out_specs=(vmem, vmem),
        scratch_shapes=[
            pltpu.VMEM((16, 8, 1024), F32), pltpu.VMEM((2, 16, 24, 128), F32),
            pltpu.VMEM((16, 24, 128), F32), pltpu.VMEM((16, 24, 128), F32), pltpu.VMEM((16, 24, 128), F32),
            pltpu.VMEM((24, 128), F32), pltpu.VMEM((8, 24, 128), F32), pltpu.VMEM((24, 128), F32), pltpu.VMEM((2, 16, 24, 128), F32),
            dma((16,)), dma((16,)), dma((2,)), dma((16,)), dma((16,)), dma((8,)), dma((8,)), dma((16,)), dma((16,)), dma((16,)), dma((16,)),
        ],
        compiler_params=pltpu.CompilerParams(collective_id=0, has_side_effects=True),
    )(slot, place(owner, arrivals), sketch)


def local(arrivals, sketch, owner, slot):
    packed, samples = collect(owner, slot.reshape(1, 128), arrivals, sketch)
    return chain(packed, sketch, samples)


def solution(mesh):
    split = Mesh(mesh.devices.reshape(2, 4, 2, 2, 8), ("grp_0", "grp_1", "grp_2", "sub_0", "sub_1"))
    placed = (P(SUB, GRP), P(None, GRP_SUB), P(GRP), P())
    return jax.shard_map(
        local,
        mesh=split,
        in_specs=placed,
        out_specs=(P(None, GRP_SUB), P(None, GRP_SUB)),
        check_vma=False,
    )
```

```python
import jax
import jax.numpy as jnp
from jax import lax
from jax.experimental import pallas as pl
from jax.experimental.pallas import tpu as pltpu
from jax.sharding import Mesh
from jax.sharding import PartitionSpec as P

SUB = ("sub_0", "sub_1")
GRP_SUB = ("grp_0", "grp_1", "grp_2", "sub_0", "sub_1")
GRP = ("grp_0", "grp_1", "grp_2")
MESH = pl.DeviceIdType.MESH

F32 = jnp.float32
HI = lax.Precision.HIGHEST
BLK = 32
HELD = 16


def nn(a, b):
    return lax.dot_general(a, b, (((1,), (0,)), ((), ())), precision=HI, preferred_element_type=F32)


def nt(a, b):
    return lax.dot_general(a, b, (((1,), (1,)), ((), ())), precision=HI, preferred_element_type=F32)


def tn(a, b):
    return lax.dot_general(a, b, (((0,), (0,)), ((), ())), precision=HI, preferred_element_type=F32)


def halves(x):
    high = x.astype(jnp.bfloat16)
    return high, (x - high.astype(F32)).astype(jnp.bfloat16)


def split_product(a, b, contracted):
    dims = (((1,), (contracted,)), ((), ()))

    def one(p, q):
        return lax.dot_general(p, q, dims, preferred_element_type=F32)

    return one(a[0], b[0]) + (one(a[0], b[1]) + one(a[1], b[0]))


def iota(shape, axis):
    return lax.broadcasted_iota(jnp.int32, shape, axis)


def spread(tile, row):
    return jnp.broadcast_to(tile[row : row + 1], (8, 128))


def pivot_block(rows, offset):
    groups = BLK // 8
    sub = iota((8, 128), 0)
    width = len(rows[0])
    roots = [None] * groups
    cols = [None] * BLK
    for k in range(BLK):
        tk, sk = divmod(k, 8)
        if k % HELD == 0:
            for j in range(k, k + HELD):
                lane = jnp.full((8, 128), j, jnp.int32) + offset
                cols[j] = [jnp.take_along_axis(rows[t][0], lane, axis=1) if t >= j // 8 else None for t in range(groups)]
            pivot = spread(cols[k][tk], sk)
        root = lax.rsqrt(pivot)
        inverse = root * root
        if (k + 1) % HELD:
            tj, sj = divmod(k + 1, 8)
            element = spread(cols[k][tj], sj)
            pivot = spread(cols[k + 1][tj], sj) - (element * element) * inverse
        scaled = [None] * groups
        for t in range(tk, groups):
            scaled[t] = cols[k][t] * inverse
        scaled[tk] = jnp.where(sub > sk, scaled[tk], 0.0)
        for j in range(k + 1, (k // HELD + 1) * HELD):
            tj, sj = divmod(j, 8)
            element = spread(cols[k][tj], sj)
            for t in range(tj, groups):
                cols[j][t] = cols[j][t] - scaled[t] * element
        for c in range(width):
            row = spread(rows[tk][c], sk)
            for t in range(tk, groups):
                rows[t][c] = rows[t][c] - scaled[t] * row
        roots[tk] = root if sk == 0 else jnp.where(sub == sk, root, roots[tk])
    for t in range(groups - 1):
        roots[t] = jnp.minimum(roots[t], roots[t] + roots[groups - 1])
    return [[tile * roots[t] for tile in rows[t]] for t in range(groups)]


def join(rows):
    return jnp.concatenate([jnp.concatenate(r, axis=1) for r in rows], axis=0)


def factor(work, last, turned, early, late):
    groups = BLK // 8

    def step(p, low, first, end):
        base = pl.multiple_of(p * BLK, BLK)
        span = slice(first * 128, end * 128)
        rows = [[work[pl.ds(base + 8 * t, 8), c * 128 : c * 128 + 128] for c in range(first, end)] for t in range(groups)]
        left = jnp.where(iota((256 - low, 128), 0) >= base + BLK - low, turned[low:, :], 0.0)[:, :BLK]
        work[low:, span] = work[low:, span] - nn(left, last[:, span])
        rows = pivot_block(rows, lax.rem(p, 4) * BLK)
        for t in range(groups):
            for c in range(first, end):
                work[pl.ds(base + 8 * t, 8), c * 128 : c * 128 + 128] = rows[t][c - first]
        panel = join(rows)
        last[:, span] = panel
        turned[low:, 0:BLK] = panel[:, low - first * 128 : 256 - first * 128].T

        @pl.when(p < 7)
        def _():
            below = pl.ds(base + BLK, BLK)
            work[below, span] = work[below, span] - nn(turned[below, 0:BLK], panel)
        return 0

    last[...] = jnp.zeros_like(last)
    turned[...] = jnp.zeros_like(turned)
    lax.fori_loop(0, 4, lambda p, _: step(p, 0, *early), 0)
    lax.fori_loop(4, 8, lambda p, _: step(p, 128, *late), 0)


def near_identity_root(excess):
    down, across = iota((256, 256), 0), iota((256, 256), 1)
    half = jnp.where(down > across, 1.0, jnp.where(down == across, 0.5, 0.0)).astype(F32)

    def onward(x):
        parts = halves(x)
        return -half * (excess + split_product(parts, parts, 1))

    def more(state):
        return (state[1] > 1e-11) & (state[2] < 64)

    def body(state):
        x = onward(state[0])
        y = onward(x)
        return y, jnp.sum((y - x) * (y - x)), state[2] + 1

    start = onward(onward(-half * excess))
    return lax.while_loop(more, body, (start, jnp.float32(1.0), jnp.int32(0)))[0]


def shrink(yt, gram, work, last, turned):
    eye = (iota((256, 256), 0) == iota((256, 256), 1)).astype(F32)
    work[:, 0:256] = nt(yt, yt)
    work[:, 256:640] = yt
    factor(work, last, turned, (0, 5), (1, 5))
    qt = work[:, 256:640]
    reduced = nt(nn(qt, gram), qt)
    work[:, 0:256] = reduced
    work[:, 256:512] = eye
    factor(work, last, turned, (0, 3), (1, 4))
    root = work[:, 256:512]
    offset = 0.5 / jnp.sum(root * root, keepdims=True)
    keeper = eye + near_identity_root(offset * tn(root, root)).T
    return nn(keeper, qt), keeper, reduced


def small(matrix, right):
    whole = jnp.concatenate([matrix, right], axis=1)
    rows = [[whole[8 * t : 8 * t + 8, c * 128 : c * 128 + 128] for c in range(whole.shape[1] // 128)] for t in range(BLK // 8)]
    return join(pivot_block(rows, 0))[:, 128:]


def square_of(a, b):
    return nt(a, jnp.concatenate([b, jnp.zeros((96, b.shape[1]), F32)], axis=0))


def chain_kernel(packed_ref, sketch_hbm, samples_hbm, final_hbm, residual_hbm, work, last, turned, gram_ref, second_gram, data_ref, outs_ref, in_sems, out_sems):
    sketch_in = pltpu.make_async_copy(sketch_hbm, data_ref.at[0:256], in_sems.at[0])
    samples_in = pltpu.make_async_copy(samples_hbm, data_ref.at[256:384], in_sems.at[1])
    sketch_in.start()
    samples_in.start()
    index = 0
    for i in range(3):
        for j in range(i + 1):
            tile = packed_ref[index * 128 : index * 128 + 128, :]
            gram_ref[i * 128 : i * 128 + 128, j * 128 : j * 128 + 128] = tile
            if i != j:
                gram_ref[j * 128 : j * 128 + 128, i * 128 : i * 128 + 128] = tile.T
            index += 1
    lanes = iota((256, 384), 1)
    yt = jnp.where(lanes < 320, gram_ref[0:256, :], 0.0)
    inner = (iota((384, 384), 0) < 320) & (iota((384, 384), 1) < 320)
    second_gram[...] = jnp.where(inner, gram_ref[...], 0.0)
    weights, keeper, reduced = shrink(yt, second_gram[...], work, last, turned)
    corner = nt(nn(keeper, reduced), keeper)
    side = pltpu.roll(nn(weights, gram_ref[:, 256:384]), 64, 1)
    side = jnp.where(iota((256, 128), 1) < 64, side, 0.0)
    tail = pltpu.roll(gram_ref[320:384, 256:384], 64, 1)
    tail = jnp.where(iota((64, 128), 1) < 64, tail, 0.0)
    second_gram[0:256, 0:256] = corner
    second_gram[0:256, 256:384] = side
    second_gram[256:384, 0:256] = side.T
    second_gram[256:320, 256:384] = tail
    second_gram[320:384, 256:384] = jnp.zeros((64, 128), F32)
    weights_two, keeper_two, reduced_two = shrink(second_gram[0:256, :], second_gram[...], work, last, turned)
    late = pltpu.roll(weights_two[:, 256:384], 64, 1)
    late = jnp.where(iota((256, 128), 1) >= 64, late, 0.0)
    whole = nn(weights_two[:, :256], weights)
    whole = jnp.concatenate([whole[:, :256], whole[:, 256:] + late], axis=1)
    sketch_in.wait()
    samples_in.wait()
    weights_parts = halves(whole)
    for i in range(4):
        at = slice(i * 256, i * 256 + 256)
        outs_ref[0:256, at] = split_product(weights_parts, halves(data_ref[:, at]), 0)
    leading = nt(nn(keeper_two[0:32], reduced_two), keeper_two)
    ut = small(square_of(leading, leading), leading)
    kept = nn(ut, keeper_two)
    towards = nn(ut, whole)
    scores = nn(towards, gram_ref[:, 256:384])
    both = small(square_of(nn(kept, reduced_two), kept), jnp.concatenate([towards, scores], axis=1))
    ident = (iota((128, 384), 1) == iota((128, 384), 0) + 256).astype(F32)
    coef = halves(ident - tn(both[:, 384:512], both[:, :384]))
    outs = [pltpu.make_async_copy(outs_ref.at[0:256], final_hbm, out_sems.at[4])]
    outs[0].start()
    for i in range(4):
        at = slice(i * 256, i * 256 + 256)
        outs_ref[256:384, at] = split_product(coef, halves(data_ref[:, at]), 0)
        outs.append(pltpu.make_async_copy(outs_ref.at[256:384, at], residual_hbm.at[:, at], out_sems.at[i]))
        outs[-1].start()
    for copy in outs:
        copy.wait()


def chain(packed, sketch, samples):
    vmem, anywhere = pl.BlockSpec(memory_space=pltpu.VMEM), pl.BlockSpec(memory_space=pl.ANY)
    square = pltpu.VMEM((384, 384), F32)
    return pl.pallas_call(
        chain_kernel,
        out_shape=(jax.ShapeDtypeStruct((256, 1024), F32), jax.ShapeDtypeStruct((128, 1024), F32)),
        in_specs=[vmem, anywhere, anywhere],
        out_specs=(anywhere, anywhere),
        scratch_shapes=[
            pltpu.VMEM((256, 640), F32), pltpu.VMEM((BLK, 640), F32), pltpu.VMEM((256, 128), F32), square, square,
            pltpu.VMEM((384, 1024), F32), pltpu.VMEM((384, 1024), F32), pltpu.SemaphoreType.DMA((2,)), pltpu.SemaphoreType.DMA((5,)),
        ],
    )(packed, sketch, samples)

def spot():
    return tuple(lax.axis_index(name) for name in GRP_SUB)


def place_tile(owner_ref, arrivals_ref, at):
    quarter = iota((8, 128), 1) // 32
    tile = None
    for i in range(4):
        host = owner_ref[at + i]
        source = arrivals_ref[host // 4]
        run = jnp.full((8, 128), host % 4, jnp.int32)
        turned = source
        for q in range(1, 4):
            turned = jnp.where(run == (i + 4 - q) % 4, pltpu.roll(source, q * 32, 1), turned)
        tile = turned if i == 0 else jnp.where(quarter == i, turned, tile)
    return tile


def collect_kernel(owner_ref, slot_ref, arrivals_ref, sketch_ref, total_ref, samples_ref,
                   placed, landed, part, twin, half, plane, piece, column, share, whole,
                   move_send, move_recv, twin_sems, plane_send, plane_recv, column_send, column_recv, share_send, share_recv, back_send, back_recv):
    y_hi, x, core, y_lo, z = spot()
    me_sub = y_lo * 8 + z
    me = (y_hi * 2 + y_lo) * 4 + x

    def in_sub(j):
        return (y_hi, x, core, j // 8, lax.rem(j, 8))

    def in_plane(q):
        y = q // 4
        return (y // 2, lax.rem(q, 4), core, lax.rem(y, 2), z)

    def in_column(k):
        return (y_hi, x, core, y_lo, k)

    other = (y_hi, x, 1 - core, y_lo, z)

    def send(source, target, send_sem, recv_sem, device):
        copy = pltpu.make_async_remote_copy(src_ref=source, dst_ref=target, send_sem=send_sem, recv_sem=recv_sem, device_id=device, device_id_type=MESH)
        copy.start()
        return copy

    barrier = pltpu.get_barrier_semaphore()
    pl.semaphore_signal(barrier, inc=1, device_id=other, device_id_type=MESH)
    for s in range(1, 16):
        pl.semaphore_signal(barrier, inc=1, device_id=in_sub(lax.rem(me_sub + s, 16)), device_id_type=MESH)
        pl.semaphore_signal(barrier, inc=1, device_id=in_plane(lax.rem(me + s, 16)), device_id_type=MESH)

    def place(peer):
        def step(i, _):
            for v in range(4):
                tile = place_tile(owner_ref, arrivals_ref, peer * 32 + i * 16 + v * 4)
                placed[peer, :, pl.ds(pl.multiple_of(i * 512 + v * 128, 128), 128)] = tile
            return 0

        lax.fori_loop(0, 2, step, 0)

    moves = []
    for s in (8, 4, 12, 3, 5, 11, 13, 2, 6, 10, 14, 1, 7, 9, 15):
        peer = lax.rem(me_sub + s, 16)
        place(peer)
        if not moves:
            pl.semaphore_wait(barrier, 31)
        moves.append(send(placed.at[peer], landed.at[me_sub], move_send.at[s], move_recv.at[s], in_sub(peer)))
    place(me_sub)
    landed[me_sub] = placed[me_sub]

    def put(index, block):
        rows = block.reshape(16, 8, 128)
        for r in range(16):
            at = index * 16 + r
            part[at // 48, (at % 48) // 3, (at % 3) * 8 : (at % 3) * 8 + 8, :] = rows[r]

    put(0, nt(sketch_ref[0:128, :], sketch_ref[0:128, :]))
    put(1, nt(sketch_ref[128:256, :], sketch_ref[0:128, :]))
    put(2, nt(sketch_ref[128:256, :], sketch_ref[128:256, :]))
    for copy in moves:
        copy.wait_recv()
    pick = (iota((128, 128), 0) == slot_ref[...]).astype(F32)
    samples_ref[...] = tn(pick, landed[...].reshape(128, 1024))
    put(3, nt(samples_ref[...], sketch_ref[0:128, :]))
    put(4, nt(samples_ref[...], sketch_ref[128:256, :]))
    put(5, nt(samples_ref[...], samples_ref[...]))

    first = send(part.at[1 - core], twin, twin_sems.at[0], twin_sems.at[1], other)
    first.wait_recv()
    half[...] = part[core] + twin[...]

    scattered = []
    for s in range(1, 16):
        peer = lax.rem(me + s, 16)
        scattered.append(send(half.at[peer], plane.at[s], plane_send.at[s], plane_recv.at[s], in_plane(peer)))
    total = half[me]
    for s in range(1, 16):
        scattered[s - 1].wait_recv()
        total = total + plane[s]
    piece[...] = total

    spread_out = []
    for s in range(1, 8):
        peer = lax.rem(z + s, 8)
        spread_out.append(send(piece, column.at[z], column_send.at[s], column_recv.at[s], in_column(peer)))
    column[z] = piece[...]
    for copy in spread_out:
        copy.wait_recv()
    total = column[0]
    for k in range(1, 8):
        total = total + column[k]
    share[...] = total

    gathered = []
    for s in range(1, 16):
        peer = lax.rem(me + s, 16)
        gathered.append(send(share, whole.at[core, me], share_send.at[s], share_recv.at[s], in_plane(peer)))
    whole[core, me] = share[...]
    back = [send(share, whole.at[core, me], back_send.at[0], back_recv.at[0], other)]
    for s in range(1, 16):
        gathered[s - 1].wait_recv()
        source = lax.rem(me + 16 - s, 16)
        back.append(send(whole.at[core, source], whole.at[core, source], back_send.at[s], back_recv.at[s], other))
    for copy in back:
        copy.wait_recv()
    total_ref[...] = whole[...].reshape(768, 128)
    for copy in moves + [first] + scattered + spread_out + gathered + back:
        copy.wait_send()


def collect(owner, slot, arrivals, sketch):
    dma = pltpu.SemaphoreType.DMA
    vmem = pl.BlockSpec(memory_space=pltpu.VMEM)
    return pl.pallas_call(
        collect_kernel,
        out_shape=(jax.ShapeDtypeStruct((768, 128), F32), jax.ShapeDtypeStruct((128, 1024), F32)),
        in_specs=[pl.BlockSpec(memory_space=pltpu.SMEM), vmem, vmem, vmem],
        out_specs=(vmem, vmem),
        scratch_shapes=[
            pltpu.VMEM((16, 8, 1024), F32), pltpu.VMEM((16, 8, 1024), F32), pltpu.VMEM((2, 16, 24, 128), F32),
            pltpu.VMEM((16, 24, 128), F32), pltpu.VMEM((16, 24, 128), F32), pltpu.VMEM((16, 24, 128), F32),
            pltpu.VMEM((24, 128), F32), pltpu.VMEM((8, 24, 128), F32), pltpu.VMEM((24, 128), F32), pltpu.VMEM((2, 16, 24, 128), F32),
            dma((16,)), dma((16,)), dma((2,)), dma((16,)), dma((16,)), dma((8,)), dma((8,)), dma((16,)), dma((16,)), dma((16,)), dma((16,)),
        ],
        compiler_params=pltpu.CompilerParams(collective_id=0, has_side_effects=True),
    )(owner, slot, arrivals.reshape(8, 128, 128).transpose(1, 0, 2), sketch)


def local(arrivals, sketch, owner, slot):
    packed, samples = collect(owner, slot.reshape(1, 128), arrivals, sketch)
    return chain(packed, sketch, samples)


def solution(mesh):
    split = Mesh(mesh.devices.reshape(2, 4, 2, 2, 8), ("grp_0", "grp_1", "grp_2", "sub_0", "sub_1"))
    placed = (P(SUB, GRP), P(None, GRP_SUB), P(GRP), P())
    return jax.shard_map(
        local,
        mesh=split,
        in_specs=placed,
        out_specs=(P(None, GRP_SUB), P(None, GRP_SUB)),
        check_vma=False,
    )
```

```python
import jax
import jax.numpy as jnp
from jax import lax
from jax.experimental import pallas as pl
from jax.experimental.pallas import tpu as pltpu
from jax.sharding import Mesh
from jax.sharding import PartitionSpec as P

SUB = ("sub_0", "sub_1")
GRP_SUB = ("grp_0", "grp_1", "grp_2", "sub_0", "sub_1")
GRP = ("grp_0", "grp_1", "grp_2")
MESH = pl.DeviceIdType.MESH

F32 = jnp.float32
HI = lax.Precision.HIGHEST
BLK = 32
HELD = 16


def nn(a, b):
    return lax.dot_general(a, b, (((1,), (0,)), ((), ())), precision=HI, preferred_element_type=F32)


def nt(a, b):
    return lax.dot_general(a, b, (((1,), (1,)), ((), ())), precision=HI, preferred_element_type=F32)


def tn(a, b):
    return lax.dot_general(a, b, (((0,), (0,)), ((), ())), precision=HI, preferred_element_type=F32)


def halves(x):
    high = x.astype(jnp.bfloat16)
    return high, (x - high.astype(F32)).astype(jnp.bfloat16)


def split_product(a, b, contracted):
    dims = (((1,), (contracted,)), ((), ()))

    def one(p, q):
        return lax.dot_general(p, q, dims, preferred_element_type=F32)

    return one(a[0], b[0]) + (one(a[0], b[1]) + one(a[1], b[0]))


def iota(shape, axis):
    return lax.broadcasted_iota(jnp.int32, shape, axis)


def spread(tile, row):
    return jnp.broadcast_to(tile[row : row + 1], (8, 128))


def pivot_block(rows, offset):
    groups = BLK // 8
    sub = iota((8, 128), 0)
    width = len(rows[0])
    roots = [None] * groups
    cols = [None] * BLK
    for k in range(BLK):
        tk, sk = divmod(k, 8)
        if k % HELD == 0:
            for j in range(k, k + HELD):
                lane = jnp.full((8, 128), j, jnp.int32) + offset
                cols[j] = [jnp.take_along_axis(rows[t][0], lane, axis=1) if t >= j // 8 else None for t in range(groups)]
            pivot = spread(cols[k][tk], sk)
        root = lax.rsqrt(pivot)
        inverse = root * root
        if (k + 1) % HELD:
            tj, sj = divmod(k + 1, 8)
            element = spread(cols[k][tj], sj)
            pivot = spread(cols[k + 1][tj], sj) - (element * element) * inverse
        scaled = [None] * groups
        for t in range(tk, groups):
            scaled[t] = cols[k][t] * inverse
        scaled[tk] = jnp.where(sub > sk, scaled[tk], 0.0)
        for j in range(k + 1, (k // HELD + 1) * HELD):
            tj, sj = divmod(j, 8)
            element = spread(cols[k][tj], sj)
            for t in range(tj, groups):
                cols[j][t] = cols[j][t] - scaled[t] * element
        for c in range(width):
            row = spread(rows[tk][c], sk)
            for t in range(tk, groups):
                rows[t][c] = rows[t][c] - scaled[t] * row
        roots[tk] = root if sk == 0 else jnp.where(sub == sk, root, roots[tk])
    for t in range(groups - 1):
        roots[t] = jnp.minimum(roots[t], roots[t] + roots[groups - 1])
    return [[tile * roots[t] for tile in rows[t]] for t in range(groups)]


def join(rows):
    return jnp.concatenate([jnp.concatenate(r, axis=1) for r in rows], axis=0)


def factor(work, last, turned, early, late):
    groups = BLK // 8

    def half(low, first, end):
        span = slice(first * 128, end * 128)
        last[...] = jnp.zeros_like(last)
        turned[...] = jnp.zeros_like(turned)

        def step(p, _):
            base = pl.multiple_of(p * BLK, BLK)
            at = pl.multiple_of(low + base, BLK)
            rows = [[work[pl.ds(at + 8 * t, 8), c * 128 : c * 128 + 128] for c in range(first, end)] for t in range(groups)]
            left = jnp.where(iota((128, 128), 0) >= base + BLK, turned[...], 0.0)[:, :BLK]
            work[low : low + 128, span] = work[low : low + 128, span] - nn(left, last[:, span])
            rows = pivot_block(rows, base)
            for t in range(groups):
                for c in range(first, end):
                    work[pl.ds(at + 8 * t, 8), c * 128 : c * 128 + 128] = rows[t][c - first]
            panel = join(rows)
            last[:, span] = panel
            turned[:, 0:BLK] = panel[:, :128].T

            @pl.when(p < 3)
            def _():
                below = pl.ds(at + BLK, BLK)
                work[below, span] = work[below, span] - nn(turned[pl.ds(base + BLK, BLK), 0:BLK], panel)
            return 0

        lax.fori_loop(0, 4, step, 0)

    half(0, *early)
    first, end = max(early[0], late[0]), min(early[1], late[1])
    span = slice(first * 128, end * 128)
    work[128:256, span] = work[128:256, span] - tn(work[0:128, 128:256], work[0:128, span])
    half(128, *late)


def near_identity_root(excess):
    down, across = iota((256, 256), 0), iota((256, 256), 1)
    half = jnp.where(down > across, 1.0, jnp.where(down == across, 0.5, 0.0)).astype(F32)

    def onward(x):
        parts = halves(x)
        return -half * (excess + split_product(parts, parts, 1))

    def more(state):
        return (state[1] > 1e-11) & (state[2] < 64)

    def body(state):
        x = onward(state[0])
        y = onward(x)
        return y, jnp.sum((y - x) * (y - x)), state[2] + 1

    start = onward(onward(-half * excess))
    return lax.while_loop(more, body, (start, jnp.float32(1.0), jnp.int32(0)))[0]


def shrink(yt, gram, work, last, turned):
    eye = (iota((256, 256), 0) == iota((256, 256), 1)).astype(F32)
    work[:, 0:256] = nt(yt, yt)
    work[:, 256:640] = yt
    factor(work, last, turned, (0, 5), (1, 5))
    qt = work[:, 256:640]
    reduced = nt(nn(qt, gram), qt)
    work[:, 0:256] = reduced
    work[:, 256:512] = eye
    factor(work, last, turned, (0, 3), (1, 4))
    root = work[:, 256:512]
    offset = 0.5 / jnp.sum(root * root, keepdims=True)
    keeper = eye + near_identity_root(offset * tn(root, root)).T
    return nn(keeper, qt), keeper, reduced


def small(matrix, right):
    whole = jnp.concatenate([matrix, right], axis=1)
    rows = [[whole[8 * t : 8 * t + 8, c * 128 : c * 128 + 128] for c in range(whole.shape[1] // 128)] for t in range(BLK // 8)]
    return join(pivot_block(rows, 0))[:, 128:]


def square_of(a, b):
    return nt(a, jnp.concatenate([b, jnp.zeros((96, b.shape[1]), F32)], axis=0))


def chain_kernel(packed_ref, sketch_hbm, samples_hbm, final_hbm, residual_hbm, work, last, turned, gram_ref, second_gram, data_ref, outs_ref, in_sems, out_sems):
    sketch_in = pltpu.make_async_copy(sketch_hbm, data_ref.at[0:256], in_sems.at[0])
    samples_in = pltpu.make_async_copy(samples_hbm, data_ref.at[256:384], in_sems.at[1])
    sketch_in.start()
    samples_in.start()
    index = 0
    for i in range(3):
        for j in range(i + 1):
            tile = packed_ref[index * 128 : index * 128 + 128, :]
            gram_ref[i * 128 : i * 128 + 128, j * 128 : j * 128 + 128] = tile
            if i != j:
                gram_ref[j * 128 : j * 128 + 128, i * 128 : i * 128 + 128] = tile.T
            index += 1
    lanes = iota((256, 384), 1)
    yt = jnp.where(lanes < 320, gram_ref[0:256, :], 0.0)
    inner = (iota((384, 384), 0) < 320) & (iota((384, 384), 1) < 320)
    second_gram[...] = jnp.where(inner, gram_ref[...], 0.0)
    weights, keeper, reduced = shrink(yt, second_gram[...], work, last, turned)
    corner = nt(nn(keeper, reduced), keeper)
    side = pltpu.roll(nn(weights, gram_ref[:, 256:384]), 64, 1)
    side = jnp.where(iota((256, 128), 1) < 64, side, 0.0)
    tail = pltpu.roll(gram_ref[320:384, 256:384], 64, 1)
    tail = jnp.where(iota((64, 128), 1) < 64, tail, 0.0)
    second_gram[0:256, 0:256] = corner
    second_gram[0:256, 256:384] = side
    second_gram[256:384, 0:256] = side.T
    second_gram[256:320, 256:384] = tail
    second_gram[320:384, 256:384] = jnp.zeros((64, 128), F32)
    weights_two, keeper_two, reduced_two = shrink(second_gram[0:256, :], second_gram[...], work, last, turned)
    late = pltpu.roll(weights_two[:, 256:384], 64, 1)
    late = jnp.where(iota((256, 128), 1) >= 64, late, 0.0)
    whole = nn(weights_two[:, :256], weights)
    whole = jnp.concatenate([whole[:, :256], whole[:, 256:] + late], axis=1)
    sketch_in.wait()
    samples_in.wait()
    weights_parts = halves(whole)
    for i in range(4):
        at = slice(i * 256, i * 256 + 256)
        outs_ref[0:256, at] = split_product(weights_parts, halves(data_ref[:, at]), 0)
    leading = nt(nn(keeper_two[0:32], reduced_two), keeper_two)
    ut = small(square_of(leading, leading), leading)
    kept = nn(ut, keeper_two)
    towards = nn(ut, whole)
    scores = nn(towards, gram_ref[:, 256:384])
    both = small(square_of(nn(kept, reduced_two), kept), jnp.concatenate([towards, scores], axis=1))
    ident = (iota((128, 384), 1) == iota((128, 384), 0) + 256).astype(F32)
    coef = halves(ident - tn(both[:, 384:512], both[:, :384]))
    outs = [pltpu.make_async_copy(outs_ref.at[0:256], final_hbm, out_sems.at[4])]
    outs[0].start()
    for i in range(4):
        at = slice(i * 256, i * 256 + 256)
        outs_ref[256:384, at] = split_product(coef, halves(data_ref[:, at]), 0)
        outs.append(pltpu.make_async_copy(outs_ref.at[256:384, at], residual_hbm.at[:, at], out_sems.at[i]))
        outs[-1].start()
    for copy in outs:
        copy.wait()


def chain(packed, sketch, samples):
    vmem, anywhere = pl.BlockSpec(memory_space=pltpu.VMEM), pl.BlockSpec(memory_space=pl.ANY)
    square = pltpu.VMEM((384, 384), F32)
    return pl.pallas_call(
        chain_kernel,
        out_shape=(jax.ShapeDtypeStruct((256, 1024), F32), jax.ShapeDtypeStruct((128, 1024), F32)),
        in_specs=[vmem, anywhere, anywhere],
        out_specs=(anywhere, anywhere),
        scratch_shapes=[
            pltpu.VMEM((256, 640), F32), pltpu.VMEM((BLK, 640), F32), pltpu.VMEM((128, 128), F32), square, square,
            pltpu.VMEM((384, 1024), F32), pltpu.VMEM((384, 1024), F32), pltpu.SemaphoreType.DMA((2,)), pltpu.SemaphoreType.DMA((5,)),
        ],
    )(packed, sketch, samples)

PLANE = ((2, 2), (2, 1), (2, 3), (1, 2), (3, 2), (2, 0), (0, 2), (1, 1), (1, 3), (3, 1), (3, 3), (1, 0), (3, 0), (0, 1), (0, 3))
COLUMN = (4, 3, 5, 2, 6, 1, 7)


def spot():
    return tuple(lax.axis_index(name) for name in GRP_SUB)


def place_tile(owner_ref, arrivals_ref, at):
    quarter = iota((8, 128), 1) // 32
    tile = None
    for i in range(4):
        host = owner_ref[at + i]
        source = arrivals_ref[host // 4]
        run = jnp.full((8, 128), host % 4, jnp.int32)
        turned = source
        for q in range(1, 4):
            turned = jnp.where(run == (i + 4 - q) % 4, pltpu.roll(source, q * 32, 1), turned)
        tile = turned if i == 0 else jnp.where(quarter == i, turned, tile)
    return tile


def collect_kernel(owner_ref, slot_ref, arrivals_ref, sketch_hbm, total_ref, samples_hbm,
                   sketch_ref, samples_ref, local_sems, placed, landed, part, twin, half, plane, piece, column, share, whole,
                   move_send, move_recv, twin_sems, plane_send, plane_recv, column_send, column_recv, share_send, share_recv, back_send, back_recv):
    y_hi, x, core, y_lo, z = spot()
    me_sub = y_lo * 8 + z
    y = y_hi * 2 + y_lo
    me = y * 4 + x
    sketch_in = pltpu.make_async_copy(sketch_hbm, sketch_ref, local_sems.at[0])
    sketch_in.start()

    def in_sub(j):
        return (y_hi, x, core, j // 8, lax.rem(j, 8))

    def over(step):
        to_y, to_x = lax.rem(y + step[0], 4), lax.rem(x + step[1], 4)
        return (to_y // 2, to_x, core, lax.rem(to_y, 2), z), to_y * 4 + to_x

    def in_column(k):
        return (y_hi, x, core, y_lo, k)

    other = (y_hi, x, 1 - core, y_lo, z)

    def send(source, target, send_sem, recv_sem, device):
        copy = pltpu.make_async_remote_copy(src_ref=source, dst_ref=target, send_sem=send_sem, recv_sem=recv_sem, device_id=device, device_id_type=MESH)
        copy.start()
        return copy

    barrier = pltpu.get_barrier_semaphore()
    pl.semaphore_signal(barrier, inc=1, device_id=other, device_id_type=MESH)
    for s in range(1, 16):
        pl.semaphore_signal(barrier, inc=1, device_id=in_sub(lax.rem(me_sub + s, 16)), device_id_type=MESH)
    for step in PLANE:
        pl.semaphore_signal(barrier, inc=1, device_id=over(step)[0], device_id_type=MESH)

    def place(peer):
        def step(i, _):
            for v in range(4):
                tile = place_tile(owner_ref, arrivals_ref, peer * 32 + i * 16 + v * 4)
                placed[peer, :, pl.ds(pl.multiple_of(i * 512 + v * 128, 128), 128)] = tile
            return 0

        lax.fori_loop(0, 2, step, 0)

    moves = []
    for s in (8, 4, 12, 3, 5, 11, 13, 2, 6, 10, 14, 1, 7, 9, 15):
        peer = lax.rem(me_sub + s, 16)
        place(peer)
        if not moves:
            pl.semaphore_wait(barrier, 31)
        moves.append(send(placed.at[peer], landed.at[me_sub], move_send.at[s], move_recv.at[s], in_sub(peer)))
    place(me_sub)
    landed[me_sub] = placed[me_sub]

    def put(index, block):
        rows = block.reshape(16, 8, 128)
        for r in range(16):
            at = index * 16 + r
            part[at // 48, (at % 48) // 3, (at % 3) * 8 : (at % 3) * 8 + 8, :] = rows[r]

    sketch_in.wait()
    put(0, nt(sketch_ref[0:128, :], sketch_ref[0:128, :]))
    put(1, nt(sketch_ref[128:256, :], sketch_ref[0:128, :]))
    put(2, nt(sketch_ref[128:256, :], sketch_ref[128:256, :]))
    for copy in moves:
        copy.wait_recv()
    pick = (iota((128, 128), 0) == slot_ref[...]).astype(F32)
    samples_ref[...] = tn(pick, landed[...].reshape(128, 1024))
    samples_out = pltpu.make_async_copy(samples_ref, samples_hbm, local_sems.at[1])
    samples_out.start()
    put(3, nt(samples_ref[...], sketch_ref[0:128, :]))
    put(4, nt(samples_ref[...], sketch_ref[128:256, :]))
    put(5, nt(samples_ref[...], samples_ref[...]))

    first = send(part.at[1 - core], twin, twin_sems.at[0], twin_sems.at[1], other)
    first.wait_recv()
    half[...] = part[core] + twin[...]

    scattered = []
    for i, step in enumerate(PLANE):
        device, peer = over(step)
        scattered.append(send(half.at[peer], plane.at[i], plane_send.at[i], plane_recv.at[i], device))
    total = half[me]
    for i in range(15):
        scattered[i].wait_recv()
        total = total + plane[i]
    piece[...] = total

    spread_out = []
    for s in COLUMN:
        spread_out.append(send(piece, column.at[z], column_send.at[s], column_recv.at[s], in_column(lax.rem(z + s, 8))))
    column[z] = piece[...]
    for copy in spread_out:
        copy.wait_recv()
    total = column[0]
    for k in range(1, 8):
        total = total + column[k]
    share[...] = total

    gathered = []
    for i, step in enumerate(PLANE):
        gathered.append(send(share, whole.at[core, me], share_send.at[i], share_recv.at[i], over(step)[0]))
    whole[core, me] = share[...]
    back = [send(share, whole.at[core, me], back_send.at[15], back_recv.at[15], other)]
    for i in range(14, -1, -1):
        step = PLANE[i]
        gathered[i].wait_recv()
        source = over((4 - step[0], 4 - step[1]))[1]
        back.append(send(whole.at[core, source], whole.at[core, source], back_send.at[i], back_recv.at[i], other))
    for copy in back:
        copy.wait_recv()
    total_ref[...] = whole[...].reshape(768, 128)
    for copy in moves + [first] + scattered + spread_out + gathered + back:
        copy.wait_send()
    samples_out.wait()


def collect(owner, slot, arrivals, sketch):
    dma = pltpu.SemaphoreType.DMA
    vmem, anywhere = pl.BlockSpec(memory_space=pltpu.VMEM), pl.BlockSpec(memory_space=pl.ANY)
    return pl.pallas_call(
        collect_kernel,
        out_shape=(jax.ShapeDtypeStruct((768, 128), F32), jax.ShapeDtypeStruct((128, 1024), F32)),
        in_specs=[pl.BlockSpec(memory_space=pltpu.SMEM), vmem, vmem, anywhere],
        out_specs=(vmem, anywhere),
        scratch_shapes=[
            pltpu.VMEM((256, 1024), F32), pltpu.VMEM((128, 1024), F32), dma((2,)),
            pltpu.VMEM((16, 8, 1024), F32), pltpu.VMEM((16, 8, 1024), F32), pltpu.VMEM((2, 16, 24, 128), F32),
            pltpu.VMEM((16, 24, 128), F32), pltpu.VMEM((16, 24, 128), F32), pltpu.VMEM((16, 24, 128), F32),
            pltpu.VMEM((24, 128), F32), pltpu.VMEM((8, 24, 128), F32), pltpu.VMEM((24, 128), F32), pltpu.VMEM((2, 16, 24, 128), F32),
            dma((16,)), dma((16,)), dma((2,)), dma((16,)), dma((16,)), dma((8,)), dma((8,)), dma((16,)), dma((16,)), dma((16,)), dma((16,)),
        ],
        compiler_params=pltpu.CompilerParams(collective_id=0, has_side_effects=True),
    )(owner, slot, arrivals.reshape(8, 128, 128).transpose(1, 0, 2), sketch)


def local(arrivals, sketch, owner, slot):
    packed, samples = collect(owner, slot.reshape(1, 128), arrivals, sketch)
    return chain(packed, sketch, samples)


def solution(mesh):
    split = Mesh(mesh.devices.reshape(2, 4, 2, 2, 8), ("grp_0", "grp_1", "grp_2", "sub_0", "sub_1"))
    placed = (P(SUB, GRP), P(None, GRP_SUB), P(GRP), P())
    return jax.shard_map(
        local,
        mesh=split,
        in_specs=placed,
        out_specs=(P(None, GRP_SUB), P(None, GRP_SUB)),
        check_vma=False,
    )
```

```python
import jax
import jax.numpy as jnp
from jax import lax
from jax.experimental import pallas as pl
from jax.experimental.pallas import tpu as pltpu
from jax.sharding import Mesh
from jax.sharding import PartitionSpec as P

SUB = ("sub_0", "sub_1")
GRP_SUB = ("grp_0", "grp_1", "grp_2", "sub_0", "sub_1")
GRP = ("grp_0", "grp_1", "grp_2")
MESH = pl.DeviceIdType.MESH

F32 = jnp.float32
HI = lax.Precision.HIGHEST
BLK = 32
HELD = 16


def nn(a, b):
    return lax.dot_general(a, b, (((1,), (0,)), ((), ())), precision=HI, preferred_element_type=F32)


def nt(a, b):
    return lax.dot_general(a, b, (((1,), (1,)), ((), ())), precision=HI, preferred_element_type=F32)


def tn(a, b):
    return lax.dot_general(a, b, (((0,), (0,)), ((), ())), precision=HI, preferred_element_type=F32)


def halves(x):
    high = x.astype(jnp.bfloat16)
    return high, (x - high.astype(F32)).astype(jnp.bfloat16)


def split_product(a, b, contracted):
    dims = (((1,), (contracted,)), ((), ()))

    def one(p, q):
        return lax.dot_general(p, q, dims, preferred_element_type=F32)

    return one(a[0], b[0]) + (one(a[0], b[1]) + one(a[1], b[0]))


def iota(shape, axis):
    return lax.broadcasted_iota(jnp.int32, shape, axis)


def spread(tile, row):
    return jnp.broadcast_to(tile[row : row + 1], (8, 128))


def pivot_block(rows, offset):
    groups = BLK // 8
    sub = iota((8, 128), 0)
    width = len(rows[0])
    roots = [None] * groups
    cols = [None] * BLK
    for k in range(BLK):
        tk, sk = divmod(k, 8)
        if k % HELD == 0:
            for j in range(k, k + HELD):
                lane = jnp.full((8, 128), j, jnp.int32) + offset
                cols[j] = [jnp.take_along_axis(rows[t][0], lane, axis=1) if t >= j // 8 else None for t in range(groups)]
            pivot = spread(cols[k][tk], sk)
        root = lax.rsqrt(pivot)
        inverse = root * root
        if (k + 1) % HELD:
            tj, sj = divmod(k + 1, 8)
            element = spread(cols[k][tj], sj)
            pivot = spread(cols[k + 1][tj], sj) - (element * element) * inverse
        scaled = [None] * groups
        for t in range(tk, groups):
            scaled[t] = cols[k][t] * inverse
        scaled[tk] = jnp.where(sub > sk, scaled[tk], 0.0)
        for j in range(k + 1, (k // HELD + 1) * HELD):
            tj, sj = divmod(j, 8)
            element = spread(cols[k][tj], sj)
            for t in range(tj, groups):
                cols[j][t] = cols[j][t] - scaled[t] * element
        for c in range(width):
            row = spread(rows[tk][c], sk)
            for t in range(tk, groups):
                rows[t][c] = rows[t][c] - scaled[t] * row
        roots[tk] = root if sk == 0 else jnp.where(sub == sk, root, roots[tk])
    for t in range(groups - 1):
        roots[t] = jnp.minimum(roots[t], roots[t] + roots[groups - 1])
    return [[tile * roots[t] for tile in rows[t]] for t in range(groups)]


def join(rows):
    return jnp.concatenate([jnp.concatenate(r, axis=1) for r in rows], axis=0)


def factor(work, last, turned, early, late):
    groups = BLK // 8

    def half(low, first, end):
        span = slice(first * 128, end * 128)
        last[...] = jnp.zeros_like(last)
        turned[...] = jnp.zeros_like(turned)

        def step(p, _):
            base = pl.multiple_of(p * BLK, BLK)
            at = pl.multiple_of(low + base, BLK)
            rows = [[work[pl.ds(at + 8 * t, 8), c * 128 : c * 128 + 128] for c in range(first, end)] for t in range(groups)]
            left = jnp.where(iota((128, 128), 0) >= base + BLK, turned[...], 0.0)[:, :BLK]
            work[low : low + 128, span] = work[low : low + 128, span] - nn(left, last[:, span])
            rows = pivot_block(rows, base)
            for t in range(groups):
                for c in range(first, end):
                    work[pl.ds(at + 8 * t, 8), c * 128 : c * 128 + 128] = rows[t][c - first]
            panel = join(rows)
            last[:, span] = panel
            turned[:, 0:BLK] = panel[:, :128].T

            @pl.when(p < 3)
            def _():
                below = pl.ds(at + BLK, BLK)
                work[below, span] = work[below, span] - nn(turned[pl.ds(base + BLK, BLK), 0:BLK], panel)
            return 0

        lax.fori_loop(0, 4, step, 0)

    half(0, *early)
    first, end = max(early[0], late[0]), min(early[1], late[1])
    span = slice(first * 128, end * 128)
    work[128:256, span] = work[128:256, span] - tn(work[0:128, 128:256], work[0:128, span])
    half(128, *late)


def near_identity_root(excess):
    down, across = iota((256, 256), 0), iota((256, 256), 1)
    half = jnp.where(down > across, 1.0, jnp.where(down == across, 0.5, 0.0)).astype(F32)

    def onward(x):
        parts = halves(x)
        return -half * (excess + split_product(parts, parts, 1))

    def more(state):
        return (state[1] > 1e-11) & (state[2] < 64)

    def body(state):
        x = onward(state[0])
        y = onward(x)
        return y, jnp.sum((y - x) * (y - x)), state[2] + 1

    start = onward(onward(-half * excess))
    return lax.while_loop(more, body, (start, jnp.float32(1.0), jnp.int32(0)))[0]


def shrink(yt, gram, work, last, turned):
    eye = (iota((256, 256), 0) == iota((256, 256), 1)).astype(F32)
    work[:, 0:256] = nt(yt, yt)
    work[:, 256:640] = yt
    factor(work, last, turned, (0, 5), (1, 5))
    qt = work[:, 256:640]
    reduced = nt(nn(qt, gram), qt)
    work[:, 0:256] = reduced
    work[:, 256:512] = eye
    factor(work, last, turned, (0, 3), (1, 4))
    root = work[:, 256:512]
    offset = 0.5 / jnp.sum(root * root, keepdims=True)
    keeper = eye + near_identity_root(offset * tn(root, root)).T
    return nn(keeper, qt), keeper, reduced


def small(matrix, right):
    whole = jnp.concatenate([matrix, right], axis=1)
    rows = [[whole[8 * t : 8 * t + 8, c * 128 : c * 128 + 128] for c in range(whole.shape[1] // 128)] for t in range(BLK // 8)]
    return join(pivot_block(rows, 0))[:, 128:]


def square_of(a, b):
    return nt(a, jnp.concatenate([b, jnp.zeros((96, b.shape[1]), F32)], axis=0))


def chain_kernel(packed_ref, sketch_hbm, samples_hbm, final_hbm, residual_hbm, work, last, turned, gram_ref, second_gram, data_ref, outs_ref, in_sems, out_sems):
    sketch_in = pltpu.make_async_copy(sketch_hbm, data_ref.at[0:256], in_sems.at[0])
    samples_in = pltpu.make_async_copy(samples_hbm, data_ref.at[256:384], in_sems.at[1])
    sketch_in.start()
    samples_in.start()
    index = 0
    for i in range(3):
        for j in range(i + 1):
            tile = packed_ref[index * 128 : index * 128 + 128, :]
            gram_ref[i * 128 : i * 128 + 128, j * 128 : j * 128 + 128] = tile
            if i != j:
                gram_ref[j * 128 : j * 128 + 128, i * 128 : i * 128 + 128] = tile.T
            index += 1
    lanes = iota((256, 384), 1)
    yt = jnp.where(lanes < 320, gram_ref[0:256, :], 0.0)
    inner = (iota((384, 384), 0) < 320) & (iota((384, 384), 1) < 320)
    second_gram[...] = jnp.where(inner, gram_ref[...], 0.0)
    weights, keeper, reduced = shrink(yt, second_gram[...], work, last, turned)
    corner = nt(nn(keeper, reduced), keeper)
    side = pltpu.roll(nn(weights, gram_ref[:, 256:384]), 64, 1)
    side = jnp.where(iota((256, 128), 1) < 64, side, 0.0)
    tail = pltpu.roll(gram_ref[320:384, 256:384], 64, 1)
    tail = jnp.where(iota((64, 128), 1) < 64, tail, 0.0)
    second_gram[0:256, 0:256] = corner
    second_gram[0:256, 256:384] = side
    second_gram[256:384, 0:256] = side.T
    second_gram[256:320, 256:384] = tail
    second_gram[320:384, 256:384] = jnp.zeros((64, 128), F32)
    weights_two, keeper_two, reduced_two = shrink(second_gram[0:256, :], second_gram[...], work, last, turned)
    late = pltpu.roll(weights_two[:, 256:384], 64, 1)
    late = jnp.where(iota((256, 128), 1) >= 64, late, 0.0)
    whole = split_product(halves(weights_two[:, :256]), halves(weights), 0)
    whole = jnp.concatenate([whole[:, :256], whole[:, 256:] + late], axis=1)
    sketch_in.wait()
    samples_in.wait()
    weights_parts = halves(whole)
    for i in range(4):
        at = slice(i * 256, i * 256 + 256)
        outs_ref[0:256, at] = split_product(weights_parts, halves(data_ref[:, at]), 0)
    outs = [pltpu.make_async_copy(outs_ref.at[0:256], final_hbm, out_sems.at[4])]
    outs[0].start()
    leading = nt(nn(keeper_two[0:32], reduced_two), keeper_two)
    ut = small(square_of(leading, leading), leading)
    kept = nn(ut, keeper_two)
    towards = nn(ut, whole)
    scores = nn(towards, gram_ref[:, 256:384])
    both = small(square_of(nn(kept, reduced_two), kept), jnp.concatenate([towards, scores], axis=1))
    ident = (iota((128, 384), 1) == iota((128, 384), 0) + 256).astype(F32)
    coef = halves(ident - tn(both[:, 384:512], both[:, :384]))
    for i in range(4):
        at = slice(i * 256, i * 256 + 256)
        outs_ref[256:384, at] = split_product(coef, halves(data_ref[:, at]), 0)
        outs.append(pltpu.make_async_copy(outs_ref.at[256:384, at], residual_hbm.at[:, at], out_sems.at[i]))
        outs[-1].start()
    for copy in outs:
        copy.wait()


def chain(packed, sketch, samples):
    vmem, anywhere = pl.BlockSpec(memory_space=pltpu.VMEM), pl.BlockSpec(memory_space=pl.ANY)
    square = pltpu.VMEM((384, 384), F32)
    return pl.pallas_call(
        chain_kernel,
        out_shape=(jax.ShapeDtypeStruct((256, 1024), F32), jax.ShapeDtypeStruct((128, 1024), F32)),
        in_specs=[vmem, anywhere, anywhere],
        out_specs=(anywhere, anywhere),
        scratch_shapes=[
            pltpu.VMEM((256, 640), F32), pltpu.VMEM((BLK, 640), F32), pltpu.VMEM((128, 128), F32), square, square,
            pltpu.VMEM((384, 1024), F32), pltpu.VMEM((384, 1024), F32), pltpu.SemaphoreType.DMA((2,)), pltpu.SemaphoreType.DMA((5,)),
        ],
        compiler_params=pltpu.CompilerParams(),
    )(packed, sketch, samples)

PLANE = ((2, 2), (2, 1), (2, 3), (1, 2), (3, 2), (2, 0), (0, 2), (1, 1), (1, 3), (3, 1), (3, 3), (1, 0), (3, 0), (0, 1), (0, 3))
COLUMN = (4, 3, 5, 2, 6, 1, 7)


def spot():
    return tuple(lax.axis_index(name) for name in GRP_SUB)


def place_tile(owner_ref, arrivals_ref, at):
    quarter = iota((8, 128), 1) // 32
    tile = None
    for i in range(4):
        host = owner_ref[at + i]
        source = arrivals_ref[host // 4]
        run = jnp.full((8, 128), host % 4, jnp.int32)
        turned = source
        for q in range(1, 4):
            turned = jnp.where(run == (i + 4 - q) % 4, pltpu.roll(source, q * 32, 1), turned)
        tile = turned if i == 0 else jnp.where(quarter == i, turned, tile)
    return tile


def collect_kernel(owner_ref, slot_ref, arrivals_ref, sketch_hbm, total_ref, samples_hbm,
                   sketch_ref, samples_ref, local_sems, placed, landed, part, twin, half, plane, piece, column, share, whole,
                   move_send, move_recv, twin_sems, plane_send, plane_recv, column_send, column_recv, share_send, share_recv, back_send, back_recv):
    y_hi, x, core, y_lo, z = spot()
    me_sub = y_lo * 8 + z
    y = y_hi * 2 + y_lo
    me = y * 4 + x
    sketch_in = pltpu.make_async_copy(sketch_hbm, sketch_ref, local_sems.at[0])
    sketch_in.start()

    def in_sub(j):
        return (y_hi, x, core, j // 8, lax.rem(j, 8))

    def over(step):
        to_y, to_x = lax.rem(y + step[0], 4), lax.rem(x + step[1], 4)
        return (to_y // 2, to_x, core, lax.rem(to_y, 2), z), to_y * 4 + to_x

    def in_column(k):
        return (y_hi, x, core, y_lo, k)

    other = (y_hi, x, 1 - core, y_lo, z)

    def send(source, target, send_sem, recv_sem, device):
        copy = pltpu.make_async_remote_copy(src_ref=source, dst_ref=target, send_sem=send_sem, recv_sem=recv_sem, device_id=device, device_id_type=MESH)
        copy.start()
        return copy

    barrier = pltpu.get_barrier_semaphore()
    pl.semaphore_signal(barrier, inc=1, device_id=other, device_id_type=MESH)
    for s in range(1, 16):
        pl.semaphore_signal(barrier, inc=1, device_id=in_sub(lax.rem(me_sub + s, 16)), device_id_type=MESH)
    for step in PLANE:
        pl.semaphore_signal(barrier, inc=1, device_id=over(step)[0], device_id_type=MESH)

    def place(peer):
        def step(i, _):
            for v in range(4):
                tile = place_tile(owner_ref, arrivals_ref, peer * 32 + i * 16 + v * 4)
                placed[peer, :, pl.ds(pl.multiple_of(i * 512 + v * 128, 128), 128)] = tile
            return 0

        lax.fori_loop(0, 2, step, 0)

    moves = []
    for s in (8, 4, 12, 3, 5, 11, 13, 2, 6, 10, 14, 1, 7, 9, 15):
        peer = lax.rem(me_sub + s, 16)
        place(peer)
        if not moves:
            pl.semaphore_wait(barrier, 31)
        moves.append(send(placed.at[peer], landed.at[me_sub], move_send.at[s], move_recv.at[s], in_sub(peer)))
    place(me_sub)
    landed[me_sub] = placed[me_sub]

    def put(index, block):
        rows = block.reshape(16, 8, 128)
        for r in range(16):
            at = index * 16 + r
            part[at // 48, (at % 48) // 3, (at % 3) * 8 : (at % 3) * 8 + 8, :] = rows[r]

    sketch_in.wait()
    put(0, nt(sketch_ref[0:128, :], sketch_ref[0:128, :]))
    put(1, nt(sketch_ref[128:256, :], sketch_ref[0:128, :]))
    put(2, nt(sketch_ref[128:256, :], sketch_ref[128:256, :]))
    for copy in moves:
        copy.wait_recv()
    pick = (iota((128, 128), 0) == slot_ref[...]).astype(F32)
    samples_ref[...] = tn(pick, landed[...].reshape(128, 1024))
    samples_out = pltpu.make_async_copy(samples_ref, samples_hbm, local_sems.at[1])
    samples_out.start()
    put(3, nt(samples_ref[...], sketch_ref[0:128, :]))
    put(4, nt(samples_ref[...], sketch_ref[128:256, :]))
    put(5, nt(samples_ref[...], samples_ref[...]))

    first = send(part.at[1 - core], twin, twin_sems.at[0], twin_sems.at[1], other)
    first.wait_recv()
    half[...] = part[core] + twin[...]

    scattered = []
    for i, step in enumerate(PLANE):
        device, peer = over(step)
        scattered.append(send(half.at[peer], plane.at[i], plane_send.at[i], plane_recv.at[i], device))
    total = half[me]
    for i in range(15):
        scattered[i].wait_recv()
        total = total + plane[i]
    piece[...] = total

    spread_out = []
    for s in COLUMN:
        spread_out.append(send(piece, column.at[z], column_send.at[s], column_recv.at[s], in_column(lax.rem(z + s, 8))))
    column[z] = piece[...]
    for copy in spread_out:
        copy.wait_recv()
    total = column[0]
    for k in range(1, 8):
        total = total + column[k]
    share[...] = total

    gathered = []
    for i, step in enumerate(PLANE):
        gathered.append(send(share, whole.at[core, me], share_send.at[i], share_recv.at[i], over(step)[0]))
    whole[core, me] = share[...]
    back = [send(share, whole.at[core, me], back_send.at[15], back_recv.at[15], other)]
    for i in range(14, -1, -1):
        step = PLANE[i]
        gathered[i].wait_recv()
        source = over((4 - step[0], 4 - step[1]))[1]
        back.append(send(whole.at[core, source], whole.at[core, source], back_send.at[i], back_recv.at[i], other))
    for copy in back:
        copy.wait_recv()
    total_ref[...] = whole[...].reshape(768, 128)
    for copy in moves + [first] + scattered + spread_out + gathered + back:
        copy.wait_send()
    samples_out.wait()


def collect(owner, slot, arrivals, sketch):
    dma = pltpu.SemaphoreType.DMA
    vmem, anywhere = pl.BlockSpec(memory_space=pltpu.VMEM), pl.BlockSpec(memory_space=pl.ANY)
    return pl.pallas_call(
        collect_kernel,
        out_shape=(jax.ShapeDtypeStruct((768, 128), F32), jax.ShapeDtypeStruct((128, 1024), F32)),
        in_specs=[pl.BlockSpec(memory_space=pltpu.SMEM), vmem, vmem, anywhere],
        out_specs=(vmem, anywhere),
        scratch_shapes=[
            pltpu.VMEM((256, 1024), F32), pltpu.VMEM((128, 1024), F32), dma((2,)),
            pltpu.VMEM((16, 8, 1024), F32), pltpu.VMEM((16, 8, 1024), F32), pltpu.VMEM((2, 16, 24, 128), F32),
            pltpu.VMEM((16, 24, 128), F32), pltpu.VMEM((16, 24, 128), F32), pltpu.VMEM((16, 24, 128), F32),
            pltpu.VMEM((24, 128), F32), pltpu.VMEM((8, 24, 128), F32), pltpu.VMEM((24, 128), F32), pltpu.VMEM((2, 16, 24, 128), F32),
            dma((16,)), dma((16,)), dma((2,)), dma((16,)), dma((16,)), dma((8,)), dma((8,)), dma((16,)), dma((16,)), dma((16,)), dma((16,)),
        ],
        compiler_params=pltpu.CompilerParams(collective_id=0, has_side_effects=True),
    )(owner, slot, arrivals.reshape(8, 128, 128).transpose(1, 0, 2), sketch)


def local(arrivals, sketch, owner, slot):
    packed, samples = collect(owner, slot.reshape(1, 128), arrivals, sketch)
    return chain(packed, sketch, samples)


def solution(mesh):
    split = Mesh(mesh.devices.reshape(2, 4, 2, 2, 8), ("grp_0", "grp_1", "grp_2", "sub_0", "sub_1"))
    placed = (P(SUB, GRP), P(None, GRP_SUB), P(GRP), P())
    return jax.shard_map(
        local,
        mesh=split,
        in_specs=placed,
        out_specs=(P(None, GRP_SUB), P(None, GRP_SUB)),
        check_vma=False,
    )
```
